512 devices in a mesh: slab: 128 (over y, z, core), cross: 4 (over x).
Axes of the slice: x: 4, y: 8, z: 8, core: 2. Of those that a mesh axis runs over, the one named last changes fastest.
Arguments:
- a_tiles: bfloat16 [1024, 7, 128, 128], P(('slab', 'cross')), may hold values from -0.1875 to 0.1875
- a_cols: int32 [1024, 7], P(('slab', 'cross')), may hold values from 0 to 17, as said below
- over_tiles: bfloat16 [2048, 128, 128], P(('slab', 'cross')), may hold values from -0.1875 to 0.1875
- over_rows: int32 [2048], P(('slab', 'cross')), may hold values from 0 to 1
- over_cols: int32 [2048], P(('slab', 'cross')), may hold values from 0 to 17
- p_tiles: bfloat16 [1024, 3, 128, 128], P(('slab', 'cross')), may hold values from -0.8984375 to 0.8984375
- p_cols: int32 [1024, 3], P(('slab', 'cross')), may hold values from 0 to 5, as said below
Outputs:
- coarse: float32 [32768, 1792], P(('slab', 'cross'))
The draws below stay inside these ranges and needn't reach their ends.
Inputs may be any that keep to these rules, and one draw needn't show every extreme that they name: `a_cols`: the 7 entries of a row are different. `p_cols`: the 3 entries of a row are different.
All inputs are finite; a program needn't handle non-finite values.
Results may differ from the reference program's by a relative error of at most 0.0063.
Values may be sent and summed in bfloat16 or wider, within the bound.
A program may use at most 64 MiB of HBM per device.

```python
import jax
import jax.numpy as jnp
from jax import lax

TILE = 128
NB = 2
K = 7
OV = 4
KP = 3
CB = 2
NT = 1024
OVT = 2048
N_SLAB = 128
N_CROSS = 4


def distinct_columns(key, rows, span, count):
    scores = jax.random.randint(key, (rows, span), 0, 2 ** 20) * span + jnp.arange(span, dtype=jnp.int32)[None, :]
    order = jnp.argsort(scores, axis=1, stable=True)
    return order[:, :count].astype(jnp.int32)


def draw_a_cols(key, part):
    return distinct_columns(jax.random.fold_in(key, 11), NT, 9 * NB, K)


def draw_p_cols(key, part):
    return distinct_columns(jax.random.fold_in(key, 23), NT, 3 * CB, KP)


def plant(entries, key, low, top_value):
    longest = entries.shape.index(max(entries.shape))
    spots = []
    for shift in (0, 1):
        where = [jax.random.randint(jax.random.fold_in(key, axis), (), 0, length) for axis, length in enumerate(entries.shape)]
        where[longest] = (where[longest] + shift) % entries.shape[longest]
        spots.append(tuple(where))
    return entries.at[spots[0]].set(low).at[spots[1]].set(top_value)


def levels(key, dims, shards, low, top_value):
    def one(dim, blocks):
        heights = jax.random.uniform(jax.random.fold_in(jax.random.fold_in(key, 6), dim), (blocks,), jnp.float32, low / len(shards), top_value / len(shards))
        return jnp.repeat(jnp.exp(heights), dims[dim] // blocks).reshape((-1,) + (1,) * (len(dims) - dim - 1))

    gain = one(*shards[0])
    for cut in shards[1:]:
        gain = gain * one(*cut)
    return gain


def centred(stream_key, shape, scale, most, split=(), kind=jnp.bfloat16):
    entries = jax.random.normal(stream_key, shape, jnp.float32) * scale
    if len(split) > 0:
        entries = levels(stream_key, shape, split, -0.22, 0.18) * entries
    return jnp.clip(entries, min=-most, max=most).astype(kind)


def setup_inputs(seed: int = 0) -> dict:
    arg_keys = jax.random.split(jax.random.key(seed), 8)
    return {
        "a_tiles": centred(arg_keys[0], (NT, K, TILE, TILE), ((K + 1) * TILE) ** -0.5, 0.1875, ((0, 512),)),
        "a_cols": draw_a_cols(jax.random.fold_in(arg_keys[7], 71), 0),
        "over_tiles": centred(arg_keys[2], (OVT, TILE, TILE), ((K + 1) * TILE) ** -0.5, 0.1875, ((0, 512),)),
        "over_rows": plant(jax.random.randint(arg_keys[3], (OVT,), 0, NB), jax.random.fold_in(arg_keys[3], 1), 0, NB - 1).astype(jnp.int32),
        "over_cols": plant(jax.random.randint(arg_keys[4], (OVT,), 0, 9 * NB), jax.random.fold_in(arg_keys[4], 1), 0, (9 * NB) - 1).astype(jnp.int32),
        "p_tiles": centred(arg_keys[5], (NT, KP, TILE, TILE), 0.15, 0.8984375, ((0, 512),)),
        "p_cols": draw_p_cols(jax.random.fold_in(arg_keys[7], 71), 0),
    }


def dense_rows(p_tiles, p_cols):
    picks = (p_cols[:, :, None] == jnp.arange(3 * CB, dtype=jnp.int32)[None, None, :]).astype(jnp.float32)
    spread = jnp.einsum("nmq,nmab->naqb", picks, p_tiles.astype(jnp.float32))
    return spread.astype(jnp.bfloat16).reshape(p_tiles.shape[0], TILE, 3 * CB * TILE)


def device_part(a_tiles, a_cols, over_tiles, over_rows, over_cols, own_rows, extended):
    width = CB * TILE
    wide = 3 * width
    product = jnp.zeros((NB, TILE, 5 * width), jnp.float32)
    for k_index in range(K):
        rows = jnp.take(extended, a_cols[:, k_index], axis=0).astype(jnp.float32)
        piece = jnp.einsum("nab,nbq->naq", a_tiles[:, k_index].astype(jnp.float32), rows)
        offsets = a_cols[:, k_index] // (3 * NB)
        for shift_index in range(3):
            mask = (offsets == shift_index).astype(jnp.float32)[:, None, None]
            product = product.at[:, :, shift_index * width:shift_index * width + wide].add(mask * piece)
    rows = jnp.take(extended, over_cols, axis=0).astype(jnp.float32)
    piece = jnp.einsum("oab,obq->oaq", over_tiles.astype(jnp.float32), rows)
    row_pick = (over_rows[:, None] == jnp.arange(NB, dtype=jnp.int32)[None, :]).astype(jnp.float32)
    offsets = over_cols // (3 * NB)
    for shift_index in range(3):
        select = row_pick * (offsets == shift_index).astype(jnp.float32)[:, None]
        contrib = jnp.einsum("on,oaq->naq", select, piece)
        product = product.at[:, :, shift_index * width:shift_index * width + wide].add(contrib)
    product = product.astype(jnp.bfloat16).reshape(NB * TILE, 5 * width)
    return lax.dot_general(own_rows, product, (((0,), (0,)), ((), ())), preferred_element_type=jnp.float32)


def reference(a_tiles, a_cols, over_tiles, over_rows, over_cols, p_tiles, p_cols):
    width = CB * TILE
    dense_p = dense_rows(p_tiles, p_cols).reshape(N_SLAB, N_CROSS, NB, TILE, 3 * width)
    padded = jnp.pad(dense_p, ((1, 1), (1, 1), (0, 0), (0, 0), (0, 0)))
    a_all = a_tiles.reshape(N_SLAB, N_CROSS, NB, K, TILE, TILE)
    ac_all = a_cols.reshape(N_SLAB, N_CROSS, NB, K)
    ov_all = over_tiles.reshape(N_SLAB, N_CROSS, OV, TILE, TILE)
    orow_all = over_rows.reshape(N_SLAB, N_CROSS, OV)
    ocol_all = over_cols.reshape(N_SLAB, N_CROSS, OV)

    def one_slab(slab_index):
        window = lax.dynamic_slice_in_dim(padded, slab_index, 3, 0)
        own_slab = lax.dynamic_index_in_dim(dense_p, slab_index, 0, keepdims=False)
        total = jnp.zeros((3 * width, 5 * width), jnp.float32)
        for part_index in range(N_CROSS):
            extended = window[:, part_index:part_index + 3].reshape(9 * NB, TILE, 3 * width)
            own_rows = own_slab[part_index].reshape(NB * TILE, 3 * width)
            total = total + device_part(a_all[slab_index, part_index], ac_all[slab_index, part_index], ov_all[slab_index, part_index], orow_all[slab_index, part_index], ocol_all[slab_index, part_index], own_rows, extended)
        return total.reshape(3, width, 5 * width)

    parts = lax.map(one_slab, jnp.arange(N_SLAB, dtype=jnp.int32))
    zero_block = jnp.zeros((1, width, 5 * width), jnp.float32)
    lower = jnp.concatenate([zero_block, parts[:-1, 2]], axis=0)
    upper = jnp.concatenate([parts[1:, 0], zero_block], axis=0)
    coarse = jnp.zeros((N_SLAB, width, 7 * width), jnp.float32)
    coarse = coarse.at[:, :, 0:5 * width].add(lower)
    coarse = coarse.at[:, :, width:6 * width].add(parts[:, 1])
    coarse = coarse.at[:, :, 2 * width:7 * width].add(upper)
    return coarse.reshape(N_SLAB * width, 7 * width)
```

```python
import functools

import jax
import jax.numpy as jnp
from jax import lax
from jax.experimental import pallas as pl
from jax.experimental.pallas import tpu as pltpu
from jax.sharding import PartitionSpec as P

CB = 2
TILE = 128
NB = 2
KP = 3
K = 7
OV = 4
WIDTH = CB * TILE
WIDE = 3 * WIDTH
PW = 5 * WIDTH
CW = 7 * WIDTH
HALF = CW // 2
TROWS = NB * KP * TILE
CROWS = NB * KP * 16
BROWS = TROWS + CROWS
F32 = jnp.float32
BF16 = jnp.bfloat16

OWN_R, OWN_L, OWN_NEAR, OWN_FAR, REL_L_NEAR, REL_L_FAR, REL_R_NEAR, REL_R_FAR = range(8)
FAR0, NEAR0 = 8, 12
X2A, X2B, X1D, X1S, X3D, X3S = range(16, 22)
N_SEMS = 22


def dot(a, b):
    return lax.dot_general(a, b, (((1,), (0,)), ((), ())), preferred_element_type=F32)


def kernel(
    n_slab, n_cross,
    a_hbm, o_hbm, p_hbm, a_cols, over_rows, over_cols, p_cols,
    out_ref,
    halo, dense, a_in, o_in, a_dense, p_turned, o_lhs, o_rhs, acc, prod,
    send_far, send_near, recv_far, recv_near, total,
    x_send, x_recv, local_sem, send_sem, recv_sem,
):
    s = lax.axis_index("slab")
    c = lax.axis_index("cross")
    core = lax.rem(s, 2)
    near = s + 1 - 2 * core
    far = s - 1 + 2 * core
    far_ok = jnp.logical_and(far >= 0, far < n_slab)
    right = lax.rem(c + 1, n_cross)
    left = lax.rem(c + n_cross - 1, n_cross)
    has_l = c > 0
    has_r = c < n_cross - 1
    r_near = 2 - 2 * core
    r_far = 2 * core
    rows = CW // 7 // n_cross

    def device(slab, cross):
        return {"slab": slab, "cross": cross}

    def remote(src, dst, i, slab, cross):
        return pltpu.make_async_remote_copy(
            src_ref=src, dst_ref=dst, send_sem=send_sem.at[i], recv_sem=recv_sem.at[i],
            device_id=device(slab, cross), device_id_type=pl.DeviceIdType.MESH,
        )

    load_p = pltpu.make_async_copy(p_hbm, halo.at[4, pl.ds(0, TROWS)], local_sem.at[0])
    load_a = pltpu.make_async_copy(a_hbm, a_in.at[:, pl.ds(0, K)], local_sem.at[1])
    load_o = pltpu.make_async_copy(o_hbm, o_in, local_sem.at[2])
    load_p.start()
    load_a.start()
    load_o.start()

    barrier = pltpu.get_barrier_semaphore()

    def greet(slab, cross):
        pl.semaphore_signal(
            barrier, inc=1, device_id=device(slab, cross), device_id_type=pl.DeviceIdType.MESH
        )

    greet(near, c)
    greet(s, left)
    greet(s, right)

    @pl.when(far_ok)
    def _():
        greet(far, c)

    for n in range(NB):
        for m in range(KP):
            number = p_cols[n, m].astype(F32)
            halo[4, pl.ds(TROWS + (n * KP + m) * 16, 16), :] = jnp.full((16, TILE), number).astype(BF16)

    nothing = jnp.full((CROWS, TILE), -1.0, BF16)

    def leave_out(b):
        halo[b, pl.ds(TROWS, CROWS), :] = nothing

    @pl.when(jnp.logical_not(has_l))
    def _():
        for r in range(3):
            leave_out(3 * r)

    @pl.when(jnp.logical_not(has_r))
    def _():
        for r in range(3):
            leave_out(3 * r + 2)

    @pl.when(jnp.logical_not(far_ok))
    def _():
        for u in range(3):
            leave_out(3 * r_far + u)
        recv_far[...] = jnp.zeros_like(recv_far)

    for n in range(NB):
        a_in[n, K] = jnp.zeros((TILE, TILE), BF16)
    acc[...] = jnp.zeros_like(acc)
    total[...] = jnp.zeros_like(total)

    pl.semaphore_wait(barrier, 3 + far_ok.astype(jnp.int32))
    load_p.wait()

    own_r = remote(halo.at[4], halo.at[3], OWN_R, s, right)
    own_l = remote(halo.at[4], halo.at[5], OWN_L, s, left)
    own_near = remote(halo.at[4], halo.at[3 * r_far + 1], OWN_NEAR, near, c)
    own_far = remote(halo.at[4], halo.at[3 * r_near + 1], OWN_FAR, far, c)
    rel_l_near = remote(halo.at[3], halo.at[3 * r_far], REL_L_NEAR, near, c)
    rel_l_far = remote(halo.at[3], halo.at[3 * r_near], REL_L_FAR, far, c)
    rel_r_near = remote(halo.at[5], halo.at[3 * r_far + 2], REL_R_NEAR, near, c)
    rel_r_far = remote(halo.at[5], halo.at[3 * r_near + 2], REL_R_FAR, far, c)

    @pl.when(has_r)
    def _():
        own_r.start()

    @pl.when(has_l)
    def _():
        own_l.start()

    @pl.when(far_ok)
    def _():
        own_far.start()

    own_near.start()

    def densify(b):
        for n in range(NB):
            tiles, marks = [], []
            for m in range(KP):
                i = n * KP + m
                tiles.append(halo[b, pl.ds(i * TILE, TILE), :].reshape(8, 16, TILE))
                marks.append(halo[b, pl.ds(TROWS + i * 16, 16), :])
            for q in range(3 * CB):
                value = jnp.zeros((8, 16, TILE), BF16)
                for m in range(KP):
                    here = jnp.broadcast_to((marks[m] == jnp.asarray(q, BF16))[None], value.shape)
                    value = jnp.where(here, tiles[m], value)
                dense[2 * b + n, :, pl.ds(q * TILE, TILE)] = value.reshape(TILE, TILE)

    densify(4)
    for n in range(NB):
        for q in range(3 * CB):
            block = dense[8 + n, :, pl.ds(q * TILE, TILE)]
            p_turned[pl.ds(q * TILE, TILE), pl.ds(n * TILE, TILE)] = block.T

    load_a.wait()
    load_o.wait()
    for n in range(NB):
        for t in range(18):
            at = jnp.int32(K)
            for k in range(K):
                at = jnp.where(a_cols[n, k] == t, k, at)
            a_dense[t // 6, pl.ds(n * TILE, TILE), pl.ds((t % 6) * TILE, TILE)] = a_in[n, at]
        for o in range(OV):
            o_lhs[pl.ds(n * TILE, TILE), pl.ds(o * TILE, TILE)] = jnp.where(
                over_rows[o] == n, o_in[o], jnp.zeros((TILE, TILE), BF16)
            )

    @pl.when(has_l)
    def _():
        own_r.wait_recv()
        rel_l_near.start()

        @pl.when(far_ok)
        def _():
            rel_l_far.start()

    @pl.when(has_r)
    def _():
        own_l.wait_recv()
        rel_r_near.start()

        @pl.when(far_ok)
        def _():
            rel_r_far.start()

    def add_slab(r):
        for j in range(3):
            right_side = dense[pl.ds(6 * r, 6), :, pl.ds(j * WIDTH, WIDTH)].reshape(WIDE, WIDTH)
            at = pl.ds(pl.multiple_of((r + j) * WIDTH, WIDTH), WIDTH)
            acc[:, at] += dot(a_dense[r], right_side)

    densify(3)
    densify(5)
    add_slab(1)

    own_near.wait_recv()

    @pl.when(has_l)
    def _():
        rel_l_near.wait_recv()

    @pl.when(has_r)
    def _():
        rel_r_near.wait_recv()

    for u in range(3):
        densify(3 * r_near + u)
    add_slab(r_near)

    @pl.when(far_ok)
    def _():
        own_far.wait_recv()

        @pl.when(has_l)
        def _():
            rel_l_far.wait_recv()

        @pl.when(has_r)
        def _():
            rel_r_far.wait_recv()

    for u in range(3):
        densify(3 * r_far + u)
    add_slab(r_far)

    for o in range(OV):
        t = over_cols[o]
        shift = (t >= 6).astype(jnp.int32) + (t >= 12).astype(jnp.int32)
        for j in range(5 * CB):
            value = jnp.zeros((TILE, TILE), BF16)
            for r in range(3):
                if 0 <= j - CB * r < 3 * CB:
                    value = jnp.where(shift == r, dense[t, :, pl.ds((j - CB * r) * TILE, TILE)], value)
            o_rhs[pl.ds(o * TILE, TILE), pl.ds(j * TILE, TILE)] = value

    for j in range(5):
        at = pl.ds(j * WIDTH, WIDTH)
        prod[:, at] = (acc[:, at] + dot(o_lhs[...], o_rhs[:, at])).astype(BF16)

    def block_rows(q):
        return p_turned[pl.ds(pl.multiple_of(q * WIDTH, WIDTH), WIDTH), :]

    order = [lax.rem(c + off, n_cross) for off in (2, 1, 3, 0)]

    def partial(q, send):
        lhs = block_rows(q)
        for j in range(5):
            at = pl.ds(j * WIDTH, WIDTH)
            send[:, :, at] = dot(lhs, prod[:, at]).astype(BF16).reshape(n_cross, rows, WIDTH)

    partial(r_far, send_far)
    far_copies = [remote(send_far.at[i], recv_far.at[i], FAR0 + k, far, c) for k, i in enumerate(order)]

    @pl.when(far_ok)
    def _():
        for copy in far_copies:
            copy.start()

    partial(r_near, send_near)
    near_copies = [remote(send_near.at[i], recv_near.at[i], NEAR0 + k, near, c) for k, i in enumerate(order)]
    for copy in near_copies:
        copy.start()

    lhs = block_rows(1)
    for j in range(5):
        total[:, :, pl.ds((j + 1) * WIDTH, WIDTH)] = dot(lhs, prod[:, pl.ds(j * WIDTH, WIDTH)]).reshape(
            n_cross, rows, WIDTH
        )

    near_at = pl.ds(pl.multiple_of((2 - 2 * core) * WIDTH, WIDTH), PW)
    far_at = pl.ds(pl.multiple_of(2 * core * WIDTH, WIDTH), PW)

    def owned(k):
        i = order[k]
        near_copies[k].wait_recv()
        total[i, :, near_at] += recv_near[i].astype(F32)

        @pl.when(far_ok)
        def _():
            far_copies[k].wait_recv()

        total[i, :, far_at] += recv_far[i].astype(F32)
        return i

    low, high = pl.ds(0, HALF), pl.ds(HALF, HALF)

    def x_copy(i, cross):
        return remote(x_send.at[i - X2A], x_recv.at[i - X2A], i, s, cross)

    x2a, x2b = x_copy(X2A, right), x_copy(X2B, left)
    x1d, x1s = x_copy(X1D, right), x_copy(X1S, right)
    x3d, x3s = x_copy(X3D, left), x_copy(X3S, left)

    i = owned(0)
    x_send[0] = total[i, :, low].astype(BF16)
    x_send[1] = total[i, :, high].astype(BF16)
    x2a.start()
    x2b.start()
    i_next = owned(1)
    x_send[2] = total[i_next, :, high].astype(BF16)
    x1d.start()
    i_last = owned(2)
    x_send[4] = total[i_last, :, low].astype(BF16)
    x3d.start()
    x2a.wait_recv()
    x_send[3] = (total[i_next, :, low] + x_recv[0].astype(F32)).astype(BF16)
    x1s.start()
    x2b.wait_recv()
    x_send[5] = (total[i_last, :, high] + x_recv[1].astype(F32)).astype(BF16)
    x3s.start()
    i = owned(3)
    x1d.wait_recv()
    x3d.wait_recv()
    x1s.wait_recv()
    out_ref[:, low] = total[i, :, low] + x_recv[3].astype(F32) + x_recv[4].astype(F32)
    x3s.wait_recv()
    out_ref[:, high] = total[i, :, high] + x_recv[2].astype(F32) + x_recv[5].astype(F32)

    own_near.wait_send()
    for copy in near_copies + [x2a, x2b, x1d, x1s, x3d, x3s]:
        copy.wait_send()

    @pl.when(has_r)
    def _():
        own_r.wait_send()
        rel_r_near.wait_send()

    @pl.when(has_l)
    def _():
        own_l.wait_send()
        rel_l_near.wait_send()

    @pl.when(far_ok)
    def _():
        own_far.wait_send()
        for copy in far_copies:
            copy.wait_send()

        @pl.when(has_r)
        def _():
            rel_r_far.wait_send()

        @pl.when(has_l)
        def _():
            rel_l_far.wait_send()


def body(n_slab, n_cross, a_tiles, a_cols, over_tiles, over_rows, over_cols, p_tiles, p_cols):
    rows = CB * TILE // n_cross
    hbm = pl.BlockSpec(memory_space=pl.ANY)
    smem = pl.BlockSpec(memory_space=pltpu.SMEM)
    return pl.pallas_call(
        functools.partial(kernel, n_slab, n_cross),
        out_shape=jax.ShapeDtypeStruct((rows, CW), F32),
        in_specs=[hbm, hbm, hbm, smem, smem, smem, smem],
        out_specs=pl.BlockSpec(memory_space=pltpu.VMEM),
        scratch_shapes=[
            pltpu.VMEM((9, BROWS, TILE), BF16),
            pltpu.VMEM((18, TILE, WIDE), BF16),
            pltpu.VMEM((NB, K + 1, TILE, TILE), BF16),
            pltpu.VMEM((OV, TILE, TILE), BF16),
            pltpu.VMEM((3, NB * TILE, WIDE), BF16),
            pltpu.VMEM((WIDE, NB * TILE), BF16),
            pltpu.VMEM((NB * TILE, OV * TILE), BF16),
            pltpu.VMEM((OV * TILE, PW), BF16),
            pltpu.VMEM((NB * TILE, PW), F32),
            pltpu.VMEM((NB * TILE, PW), BF16),
            pltpu.VMEM((n_cross, rows, PW), BF16),
            pltpu.VMEM((n_cross, rows, PW), BF16),
            pltpu.VMEM((n_cross, rows, PW), BF16),
            pltpu.VMEM((n_cross, rows, PW), BF16),
            pltpu.VMEM((n_cross, rows, CW), F32),
            pltpu.VMEM((6, rows, HALF), BF16),
            pltpu.VMEM((6, rows, HALF), BF16),
            pltpu.SemaphoreType.DMA((3,)),
            pltpu.SemaphoreType.DMA((N_SEMS,)),
            pltpu.SemaphoreType.DMA((N_SEMS,)),
        ],
        compiler_params=pltpu.CompilerParams(collective_id=0, has_side_effects=True),
    )(a_tiles, over_tiles, p_tiles.reshape(TROWS, TILE), a_cols, over_rows, over_cols, p_cols)


def solution(mesh):
    return jax.shard_map(
        functools.partial(body, mesh.shape["slab"], mesh.shape["cross"]),
        mesh=mesh,
        in_specs=(
            P(("slab", "cross"), None, None, None),
            P(("slab", "cross"), None),
            P(("slab", "cross"), None, None),
            P(("slab", "cross")),
            P(("slab", "cross")),
            P(("slab", "cross"), None, None, None),
            P(("slab", "cross"), None),
        ),
        out_specs=P(("slab", "cross"), None),
        check_vma=False,
    )
```

```python
import functools

import jax
import jax.numpy as jnp
from jax import lax
from jax.experimental import pallas as pl
from jax.experimental.pallas import tpu as pltpu
from jax.sharding import PartitionSpec as P

CB = 2
TILE = 128
NB = 2
KP = 3
K = 7
OV = 4
WIDTH = CB * TILE
WIDE = 3 * WIDTH
PW = 5 * WIDTH
CW = 7 * WIDTH
EARLY = CW - PW
NCH = 3
TPC = NB * KP // NCH
TROWS = TPC * TILE
BROWS = TROWS + 16
F32 = jnp.float32
BF16 = jnp.bfloat16

OWN_R, OWN_L, OWN_NEAR, OWN_FAR, REL_L_NEAR, REL_L_FAR, REL_R_NEAR, REL_R_FAR = (NCH * i for i in range(8))
FAR0 = 8 * NCH
NEAR0 = FAR0 + 5
X0 = NEAR0 + 4
N_SEMS = X0 + 16


def dot(a, b):
    return lax.dot_general(a, b, (((1,), (0,)), ((), ())), preferred_element_type=F32)


def kernel(
    n_slab, n_cross,
    a_hbm, o_hbm, p_hbm, a_cols, over_rows, over_cols, p_cols,
    out_ref,
    halo, dense, a_in, o_in, a_dense, p_turned, acc, prod,
    send_far, send_near, recv_far, recv_near, total,
    e_send, e_recv, x_send, x_recv, local_sem, send_sem, recv_sem,
):
    s = lax.axis_index("slab")
    c = lax.axis_index("cross")
    core = lax.rem(s, 2)
    near = s + 1 - 2 * core
    far = s - 1 + 2 * core
    far_ok = jnp.logical_and(far >= 0, far < n_slab)
    right = lax.rem(c + 1, n_cross)
    left = lax.rem(c + n_cross - 1, n_cross)
    has_l = c > 0
    has_r = c < n_cross - 1
    r_near = 2 - 2 * core
    r_far = 2 * core
    rows = CB * TILE // n_cross
    part_rows = rows // 2

    def device(slab, cross):
        return {"slab": slab, "cross": cross}

    def remote(src, dst, i, slab, cross):
        return pltpu.make_async_remote_copy(
            src_ref=src, dst_ref=dst, send_sem=send_sem.at[i], recv_sem=recv_sem.at[i],
            device_id=device(slab, cross), device_id_type=pl.DeviceIdType.MESH,
        )

    load_p = [
        pltpu.make_async_copy(
            p_hbm.at[pl.ds(h * TROWS, TROWS)], halo.at[4, h, pl.ds(0, TROWS)], local_sem.at[2 + h]
        )
        for h in range(NCH)
    ]
    load_a = pltpu.make_async_copy(a_hbm, a_in.at[:, pl.ds(0, K)], local_sem.at[0])
    load_o = pltpu.make_async_copy(o_hbm, o_in.at[pl.ds(0, OV)], local_sem.at[1])
    for load in load_p + [load_a, load_o]:
        load.start()

    barrier = pltpu.get_barrier_semaphore()

    def greet(slab, cross):
        pl.semaphore_signal(
            barrier, inc=1, device_id=device(slab, cross), device_id_type=pl.DeviceIdType.MESH
        )

    @pl.when(far_ok)
    def _():
        greet(far, c)

    greet(s, left)
    greet(s, right)
    greet(near, c)

    row = lax.broadcasted_iota(jnp.int32, (16, TILE), 0)
    for h in range(NCH):
        value = jnp.full((16, TILE), -1.0, F32)
        for j in range(TPC):
            n, m = divmod(h * TPC + j, KP)
            value = jnp.where(row == j, p_cols[n, m].astype(F32), value)
        halo[4, h, pl.ds(TROWS, 16), :] = value.astype(BF16)

    nothing = jnp.full((16, TILE), -1.0, BF16)

    def leave_out(b):
        for h in range(NCH):
            halo[b, h, pl.ds(TROWS, 16), :] = nothing

    @pl.when(jnp.logical_not(has_l))
    def _():
        for r in range(3):
            leave_out(3 * r)

    @pl.when(jnp.logical_not(has_r))
    def _():
        for r in range(3):
            leave_out(3 * r + 2)

    @pl.when(jnp.logical_not(far_ok))
    def _():
        for u in range(3):
            leave_out(3 * r_far + u)
        recv_far[...] = jnp.zeros_like(recv_far)

    for n in range(NB):
        a_in[n, K] = jnp.zeros((TILE, TILE), BF16)
    o_in[OV] = jnp.zeros((TILE, TILE), BF16)
    acc[...] = jnp.zeros_like(acc)
    total[...] = jnp.zeros_like(total)

    pl.semaphore_wait(barrier, 3 + far_ok.astype(jnp.int32))

    def halo_copies(b, to, first, slab, cross):
        return [remote(halo.at[b, h], halo.at[to, h], first + h, slab, cross) for h in range(NCH)]

    own_r = halo_copies(4, 3, OWN_R, s, right)
    own_l = halo_copies(4, 5, OWN_L, s, left)
    own_near = halo_copies(4, 3 * r_far + 1, OWN_NEAR, near, c)
    own_far = halo_copies(4, 3 * r_near + 1, OWN_FAR, far, c)
    rel_l_near = halo_copies(3, 3 * r_far, REL_L_NEAR, near, c)
    rel_l_far = halo_copies(3, 3 * r_near, REL_L_FAR, far, c)
    rel_r_near = halo_copies(5, 3 * r_far + 2, REL_R_NEAR, near, c)
    rel_r_far = halo_copies(5, 3 * r_near + 2, REL_R_FAR, far, c)

    for h in range(NCH):
        load_p[h].wait()

        @pl.when(has_r)
        def _():
            own_r[h].start()

        @pl.when(has_l)
        def _():
            own_l[h].start()

        @pl.when(far_ok)
        def _():
            own_far[h].start()

        own_near[h].start()

    def densify(b):
        for n in range(NB):
            tiles, marks = [], []
            for m in range(KP):
                h, j = divmod(n * KP + m, TPC)
                tiles.append(halo[b, h, pl.ds(j * TILE, TILE), :].reshape(8, 16, TILE))
                number = halo[b, h, pl.ds(TROWS, 16), :].astype(F32)[j : j + 1]
                marks.append(jnp.broadcast_to(number, (16, TILE)).astype(BF16))
            for q in range(3 * CB):
                value = jnp.zeros((8, 16, TILE), BF16)
                for m in range(KP):
                    here = jnp.broadcast_to((marks[m] == jnp.asarray(q, BF16))[None], value.shape)
                    value = jnp.where(here, tiles[m], value)
                dense[2 * b + n, :, pl.ds(q * TILE, TILE)] = value.reshape(TILE, TILE)

    def place_a(r):
        for n in range(NB):
            for t in range(6 * r, 6 * r + 6):
                at = jnp.int32(K)
                for k in range(K):
                    at = jnp.where(a_cols[n, k] == t, k, at)
                value = a_in[n, at].astype(F32)
                for o in range(OV):
                    hit = jnp.logical_and(over_rows[o] == n, over_cols[o] == t)
                    value += o_in[jnp.where(hit, o, OV)].astype(F32)
                a_dense[r, pl.ds(n * TILE, TILE), pl.ds((t % 6) * TILE, TILE)] = value.astype(BF16)

    def relay(h):
        @pl.when(has_l)
        def _():
            own_r[h].wait_recv()

            @pl.when(far_ok)
            def _():
                rel_l_far[h].start()

            rel_l_near[h].start()

        @pl.when(has_r)
        def _():
            own_l[h].wait_recv()

            @pl.when(far_ok)
            def _():
                rel_r_far[h].start()

            rel_r_near[h].start()

    def product_of(r, u, count, j):
        right_side = dense[pl.ds(6 * r + 2 * u, 2 * count), :, pl.ds(j * WIDTH, WIDTH)]
        return dot(
            a_dense[r, :, pl.ds(u * WIDTH, count * WIDTH)], right_side.reshape(count * WIDTH, WIDTH)
        )

    def columns(r, j):
        return pl.ds(pl.multiple_of((r + j) * WIDTH, WIDTH), WIDTH)

    def add_blocks(r, u, count):
        for j in range(3):
            acc[:, columns(r, j)] += product_of(r, u, count, j)

    densify(4)
    for n in range(NB):
        for q in range(3 * CB):
            block = dense[8 + n, :, pl.ds(q * TILE, TILE)]
            p_turned[pl.ds(q * TILE, TILE), pl.ds(n * TILE, TILE)] = block.T
    load_a.wait()
    load_o.wait()
    place_a(1)
    relay(0)
    place_a(0)
    relay(1)
    place_a(2)
    for h in range(2, NCH):
        relay(h)
    densify(3)
    densify(5)
    add_blocks(1, 0, 3)

    for h in range(NCH):
        own_near[h].wait_recv()

    @pl.when(has_l)
    def _():
        for h in range(NCH):
            rel_l_near[h].wait_recv()

    @pl.when(has_r)
    def _():
        for h in range(NCH):
            rel_r_near[h].wait_recv()

    for u in range(3):
        densify(3 * r_near + u)
    add_blocks(r_near, 0, 3)
    for j in range(2):
        at = pl.ds(pl.multiple_of((3 - 3 * core + j) * WIDTH, WIDTH), WIDTH)
        prod[:, at] = acc[:, at].astype(BF16)

    @pl.when(far_ok)
    def _():
        for h in range(NCH):
            own_far[h].wait_recv()

    densify(3 * r_far + 1)
    add_blocks(r_far, 1, 1)

    @pl.when(jnp.logical_and(far_ok, has_l))
    def _():
        for h in range(NCH):
            rel_l_far[h].wait_recv()

    densify(3 * r_far)
    add_blocks(r_far, 0, 1)

    @pl.when(jnp.logical_and(far_ok, has_r))
    def _():
        for h in range(NCH):
            rel_r_far[h].wait_recv()

    densify(3 * r_far + 2)
    for j in range(3):
        at = columns(r_far, j)
        prod[:, at] = (acc[:, at] + product_of(r_far, 2, 1, j)).astype(BF16)

    order = [lax.rem(c + off, n_cross) for off in (2, 1, 3, 0)]

    def chunk_of(q, k, j):
        lhs = p_turned[pl.ds(pl.multiple_of(q * WIDTH + order[k] * rows, rows), rows), :]
        return dot(lhs, prod[:, pl.ds(j * WIDTH, WIDTH)])

    first_half, second_half = pl.ds(0, part_rows), pl.ds(part_rows, part_rows)
    far_copies = [
        remote(send_far.at[0, half], recv_far.at[0, half], FAR0 + i, far, c)
        for i, half in enumerate((first_half, second_half))
    ]
    far_copies += [remote(send_far.at[k], recv_far.at[k], FAR0 + 1 + k, far, c) for k in range(1, 4)]
    near_copies = [remote(send_near.at[k], recv_near.at[k], NEAR0 + k, near, c) for k in range(4)]

    def send_far_chunk(k):
        for j in range(5):
            send_far[k, :, pl.ds(j * WIDTH, WIDTH)] = chunk_of(r_far, k, j).astype(BF16)

        @pl.when(far_ok)
        def _():
            for copy in far_copies[:2] if k == 0 else [far_copies[k + 1]]:
                copy.start()

    def send_near_chunk(k):
        for j in range(5):
            send_near[k, :, pl.ds(j * WIDTH, WIDTH)] = chunk_of(r_near, k, j).astype(BF16)
        near_copies[k].start()

    def own_chunk(k):
        for j in range(5):
            total[k, :, pl.ds((j + 1) * WIDTH, WIDTH)] = chunk_of(1, k, j)

    send_far_chunk(0)
    send_near_chunk(0)
    send_far_chunk(1)
    send_near_chunk(1)
    send_near_chunk(2)
    own_chunk(0)
    send_far_chunk(2)
    send_far_chunk(3)
    send_near_chunk(3)
    for k in range(1, 4):
        own_chunk(k)

    near_at = pl.ds(pl.multiple_of((2 - 2 * core) * WIDTH, WIDTH), PW)
    far_at = pl.ds(pl.multiple_of(2 * core * WIDTH, WIDTH), PW)
    everything = pl.ds(0, rows)

    def add_near(k):
        near_copies[k].wait_recv()
        total[k, :, near_at] += recv_near[k].astype(F32)

    def add_far(k, i, here):
        @pl.when(far_ok)
        def _():
            far_copies[i].wait_recv()

        total[k, here, far_at] += recv_far[k, here, :].astype(F32)

    early_first = pl.multiple_of((5 - 5 * core) * WIDTH, WIDTH)
    late_first = pl.multiple_of(2 * core * WIDTH, WIDTH)
    early = [pl.ds(pl.multiple_of(early_first + i * (EARLY // 2), TILE), EARLY // 2) for i in range(2)]
    late = [pl.ds(pl.multiple_of(late_first + i * (PW // 2), TILE), PW // 2) for i in range(2)]

    to = [right, left]

    def early_copy(step, side):
        i = 2 * step + side
        return remote(e_send.at[i], e_recv.at[i], X0 + i, s, to[side])

    def late_copy(step, side, here, extra):
        i = 2 * step + side
        return remote(x_send.at[i, here], x_recv.at[i, here], X0 + 6 + extra + side, s, to[side])

    e = [[early_copy(step, side) for side in range(2)] for step in range(3)]
    halves = (first_half, second_half)
    x_two = [[late_copy(0, side, here, 2 * i) for side in range(2)] for i, here in enumerate(halves)]
    x_alone = [late_copy(1, side, everything, 4) for side in range(2)]
    x_sum = [[late_copy(2, side, here, 6 + 2 * i) for side in range(2)] for i, here in enumerate(halves)]

    add_near(0)
    for side in range(2):
        e_send[side] = total[0, :, early[side]].astype(BF16)
        e[0][side].start()
    for side in range(2):
        add_near(1 + side)
        e_send[2 + side] = total[1 + side, :, early[1 - side]].astype(BF16)
        e[1][side].start()
    for i, here in enumerate(halves):
        add_far(0, i, here)
        for side in range(2):
            x_send[side, here, :] = total[0, here, late[side]].astype(BF16)
            x_two[i][side].start()
    for side in range(2):
        e[0][side].wait_recv()
        e_send[4 + side] = (total[1 + side, :, early[side]] + e_recv[side].astype(F32)).astype(BF16)
        e[2][side].start()
    for side in range(2):
        add_far(1 + side, 2 + side, everything)
        x_send[2 + side] = total[1 + side, :, late[1 - side]].astype(BF16)
        x_alone[side].start()
    for i, here in enumerate(halves):
        for side in range(2):
            x_two[i][side].wait_recv()
            x_send[4 + side, here, :] = (
                total[1 + side, here, late[side]] + x_recv[side, here, :].astype(F32)
            ).astype(BF16)
            x_sum[i][side].start()
    add_near(3)
    add_far(3, 4, everything)
    for side in range(2):
        e[1][side].wait_recv()
        e[2][side].wait_recv()
    for side in range(2):
        out_ref[:, early[side]] = (
            total[3, :, early[side]] + e_recv[4 + side].astype(F32) + e_recv[3 - side].astype(F32)
        )
    for side in range(2):
        x_alone[side].wait_recv()
    for side in range(2):
        total[3, :, late[side]] += x_recv[3 - side].astype(F32)
    for i, here in enumerate(halves):
        for side in range(2):
            x_sum[i][side].wait_recv()
            out_ref[here, late[side]] = total[3, here, late[side]] + x_recv[4 + side, here, :].astype(F32)

    for copy in own_near + near_copies + e[0] + e[1] + e[2] + x_two[0] + x_two[1] + x_alone + x_sum[0] + x_sum[1]:
        copy.wait_send()

    @pl.when(has_r)
    def _():
        for copy in own_r + rel_r_near:
            copy.wait_send()

    @pl.when(has_l)
    def _():
        for copy in own_l + rel_l_near:
            copy.wait_send()

    @pl.when(far_ok)
    def _():
        for copy in own_far + far_copies:
            copy.wait_send()

        @pl.when(has_r)
        def _():
            for copy in rel_r_far:
                copy.wait_send()

        @pl.when(has_l)
        def _():
            for copy in rel_l_far:
                copy.wait_send()


def body(n_slab, n_cross, a_tiles, a_cols, over_tiles, over_rows, over_cols, p_tiles, p_cols):
    rows = CB * TILE // n_cross
    hbm = pl.BlockSpec(memory_space=pl.ANY)
    smem = pl.BlockSpec(memory_space=pltpu.SMEM)
    return pl.pallas_call(
        functools.partial(kernel, n_slab, n_cross),
        out_shape=jax.ShapeDtypeStruct((rows, CW), F32),
        in_specs=[hbm, hbm, hbm, smem, smem, smem, smem],
        out_specs=pl.BlockSpec(memory_space=pltpu.VMEM),
        scratch_shapes=[
            pltpu.VMEM((9, NCH, BROWS, TILE), BF16),
            pltpu.VMEM((18, TILE, WIDE), BF16),
            pltpu.VMEM((NB, K + 1, TILE, TILE), BF16),
            pltpu.VMEM((OV + 1, TILE, TILE), BF16),
            pltpu.VMEM((3, NB * TILE, WIDE), BF16),
            pltpu.VMEM((WIDE, NB * TILE), BF16),
            pltpu.VMEM((NB * TILE, PW), F32),
            pltpu.VMEM((NB * TILE, PW), BF16),
            pltpu.VMEM((n_cross, rows, PW), BF16),
            pltpu.VMEM((n_cross, rows, PW), BF16),
            pltpu.VMEM((n_cross, rows, PW), BF16),
            pltpu.VMEM((n_cross, rows, PW), BF16),
            pltpu.VMEM((n_cross, rows, CW), F32),
            pltpu.VMEM((6, rows, EARLY // 2), BF16),
            pltpu.VMEM((6, rows, EARLY // 2), BF16),
            pltpu.VMEM((6, rows, PW // 2), BF16),
            pltpu.VMEM((6, rows, PW // 2), BF16),
            pltpu.SemaphoreType.DMA((2 + NCH,)),
            pltpu.SemaphoreType.DMA((N_SEMS,)),
            pltpu.SemaphoreType.DMA((N_SEMS,)),
        ],
        compiler_params=pltpu.CompilerParams(collective_id=0, has_side_effects=True),
    )(a_tiles, over_tiles, p_tiles.reshape(NB * KP * TILE, TILE), a_cols, over_rows, over_cols, p_cols)


def solution(mesh):
    return jax.shard_map(
        functools.partial(body, mesh.shape["slab"], mesh.shape["cross"]),
        mesh=mesh,
        in_specs=(
            P(("slab", "cross"), None, None, None),
            P(("slab", "cross"), None),
            P(("slab", "cross"), None, None),
            P(("slab", "cross")),
            P(("slab", "cross")),
            P(("slab", "cross"), None, None, None),
            P(("slab", "cross"), None),
        ),
        out_specs=P(("slab", "cross"), None),
        check_vma=False,
    )
```

```python
import functools

import jax
import jax.numpy as jnp
from jax import lax
from jax.experimental import pallas as pl
from jax.experimental.pallas import tpu as pltpu
from jax.sharding import PartitionSpec as P

CB = 2
TILE = 128
NB = 2
KP = 3
K = 7
OV = 4
WIDTH = CB * TILE
WIDE = 3 * WIDTH
PW = 5 * WIDTH
CW = 7 * WIDTH
EARLY = CW - PW
NCH = NB * KP
MARKS = 16
BROWS = MARKS + NCH * TILE
RELAYED = (0, 1, 2, 3)
TURNED = (4, 5)
F32 = jnp.float32
BF16 = jnp.bfloat16

OWN_R, OWN_L, OWN_NEAR, OWN_FAR, REL_L_NEAR, REL_L_FAR, REL_R_NEAR, REL_R_FAR, TURN_R, TURN_L = (
    NCH * i for i in range(10)
)
FAR0 = 10 * NCH
NEAR0 = FAR0 + 9
X0 = NEAR0 + 4
N_SEMS = X0 + 16


def dot(a, b):
    return lax.dot_general(a, b, (((1,), (0,)), ((), ())), preferred_element_type=F32)


def kernel(
    n_slab, n_cross,
    a_hbm, o_hbm, p_hbm, a_cols_hbm, over_rows_hbm, over_cols_hbm, p_cols_hbm,
    out_ref,
    a_cols, over_rows, over_cols, p_cols,
    halo, dense, a_in, o_in, a_dense, p_turned, acc, prod,
    send_far, send_near, recv_far, recv_near, total,
    e_send, e_recv, x_send, x_recv, local_sem, send_sem, recv_sem,
):
    s = lax.axis_index("slab")
    c = lax.axis_index("cross")
    core = lax.rem(s, 2)
    near = s + 1 - 2 * core
    far = s - 1 + 2 * core
    far_ok = jnp.logical_and(far >= 0, far < n_slab)
    right = lax.rem(c + 1, n_cross)
    left = lax.rem(c + n_cross - 1, n_cross)
    has_l = c > 0
    has_r = c < n_cross - 1
    r_near = 2 - 2 * core
    r_far = 2 * core
    rows = CB * TILE // n_cross
    part_rows = rows // 2

    def device(slab, cross):
        return {"slab": slab, "cross": cross}

    def remote(src, dst, i, slab, cross):
        return pltpu.make_async_remote_copy(
            src_ref=src, dst_ref=dst, send_sem=send_sem.at[i], recv_sem=recv_sem.at[i],
            device_id=device(slab, cross), device_id_type=pl.DeviceIdType.MESH,
        )

    barrier = pltpu.get_barrier_semaphore()

    def greet(slab, cross):
        pl.semaphore_signal(
            barrier, inc=1, device_id=device(slab, cross), device_id_type=pl.DeviceIdType.MESH
        )

    @pl.when(far_ok)
    def _():
        greet(far, c)

    greet(s, left)
    greet(s, right)
    greet(near, c)

    load_p = pltpu.make_async_copy(p_hbm, halo.at[4, pl.ds(MARKS, NCH * TILE)], local_sem.at[0])
    load_numbers = pltpu.make_async_copy(p_cols_hbm, p_cols, local_sem.at[1])
    load_a = [
        pltpu.make_async_copy(a_hbm, a_in.at[:, pl.ds(0, K)], local_sem.at[2]),
        pltpu.make_async_copy(a_cols_hbm, a_cols, local_sem.at[3]),
        pltpu.make_async_copy(o_hbm, o_in.at[pl.ds(0, OV)], local_sem.at[4]),
        pltpu.make_async_copy(over_rows_hbm, over_rows, local_sem.at[5]),
        pltpu.make_async_copy(over_cols_hbm, over_cols, local_sem.at[6]),
    ]
    for load in [load_numbers, load_p] + load_a:
        load.start()

    nothing = jnp.full((MARKS, TILE), -1.0, BF16)

    def leave_out(b):
        halo[b, pl.ds(0, MARKS), :] = nothing

    @pl.when(jnp.logical_not(has_l))
    def _():
        for r in range(3):
            leave_out(3 * r)

    @pl.when(jnp.logical_not(has_r))
    def _():
        for r in range(3):
            leave_out(3 * r + 2)

    @pl.when(jnp.logical_not(far_ok))
    def _():
        for u in range(3):
            leave_out(3 * r_far + u)
        recv_far[...] = jnp.zeros_like(recv_far)

    for n in range(NB):
        a_in[n, K] = jnp.zeros((TILE, TILE), BF16)
    o_in[OV] = jnp.zeros((TILE, TILE), BF16)
    acc[...] = jnp.zeros_like(acc)
    total[...] = jnp.zeros_like(total)

    load_numbers.wait()
    row = lax.broadcasted_iota(jnp.int32, (MARKS, TILE), 0)
    value = jnp.full((MARKS, TILE), -1.0, F32)
    for i in range(NCH):
        value = jnp.where(row == i, p_cols[i // KP, i % KP].astype(F32), value)
    halo[4, pl.ds(0, MARKS), :] = value.astype(BF16)
    load_p.wait()
    pl.semaphore_wait(barrier, 3 + far_ok.astype(jnp.int32))

    def halo_copies(b, to, first, slab, cross, chunks=range(NCH)):
        copies = {}
        for h in chunks:
            at = pl.ds(0, MARKS + TILE) if h == 0 else pl.ds(MARKS + h * TILE, TILE)
            copies[h] = remote(halo.at[b, at], halo.at[to, at], first + h, slab, cross)
        return copies

    own_r = halo_copies(4, 3, OWN_R, s, right)
    own_l = halo_copies(4, 5, OWN_L, s, left)
    own_near = halo_copies(4, 3 * r_far + 1, OWN_NEAR, near, c)
    own_far = halo_copies(4, 3 * r_near + 1, OWN_FAR, far, c)
    rel_l_near = halo_copies(3, 3 * r_far, REL_L_NEAR, near, c)
    rel_l_far = halo_copies(3, 3 * r_near, REL_L_FAR, far, c, RELAYED)
    rel_r_near = halo_copies(5, 3 * r_far + 2, REL_R_NEAR, near, c)
    rel_r_far = halo_copies(5, 3 * r_near + 2, REL_R_FAR, far, c, RELAYED)
    turn_r = halo_copies(3 * r_far + 1, 3 * r_far, TURN_R, s, right, TURNED)
    turn_l = halo_copies(3 * r_far + 1, 3 * r_far + 2, TURN_L, s, left, TURNED)

    for h in range(NCH):

        @pl.when(has_r)
        def _():
            own_r[h].start()

        @pl.when(has_l)
        def _():
            own_l[h].start()

    @pl.when(far_ok)
    def _():
        for h in TURNED + RELAYED:
            own_far[h].start()

    for h in range(NCH):
        own_near[h].start()

    def densify(b):
        for n in range(NB):
            tiles, marks = [], []
            numbers = halo[b, pl.ds(0, MARKS), :].astype(F32)
            for i in range(n * KP, n * KP + KP):
                tiles.append(halo[b, pl.ds(MARKS + i * TILE, TILE), :].reshape(8, 16, TILE))
                marks.append(jnp.broadcast_to(numbers[i : i + 1], (16, TILE)).astype(BF16))
            for q in range(3 * CB):
                value = jnp.zeros((8, 16, TILE), BF16)
                for m in range(KP):
                    here = jnp.broadcast_to((marks[m] == jnp.asarray(q, BF16))[None], value.shape)
                    value = jnp.where(here, tiles[m], value)
                dense[2 * b + n, :, pl.ds(q * TILE, TILE)] = value.reshape(TILE, TILE)

    def place_a(r, places=(0, 1)):
        for n in places:
            for t in range(6 * r, 6 * r + 6):
                at = jnp.int32(K)
                for k in range(K):
                    at = jnp.where(a_cols[n, k] == t, k, at)
                value = a_in[n, at].astype(F32)
                for o in range(OV):
                    hit = jnp.logical_and(over_rows[o] == n, over_cols[o] == t)
                    value += o_in[jnp.where(hit, o, OV)].astype(F32)
                a_dense[r, pl.ds(n * TILE, TILE), pl.ds((t % 6) * TILE, TILE)] = value.astype(BF16)

    def relay(h):
        @pl.when(has_l)
        def _():
            own_r[h].wait_recv()
            if h in RELAYED:

                @pl.when(far_ok)
                def _():
                    rel_l_far[h].start()

            rel_l_near[h].start()

        @pl.when(has_r)
        def _():
            own_l[h].wait_recv()
            if h in RELAYED:

                @pl.when(far_ok)
                def _():
                    rel_r_far[h].start()

            rel_r_near[h].start()

    def turn(h):
        @pl.when(far_ok)
        def _():
            own_far[h].wait_recv()

            @pl.when(has_r)
            def _():
                turn_r[h].start()

            @pl.when(has_l)
            def _():
                turn_l[h].start()

    def product_of(r, u, count, j):
        right_side = dense[pl.ds(6 * r + 2 * u, 2 * count), :, pl.ds(j * WIDTH, WIDTH)]
        return dot(
            a_dense[r, :, pl.ds(u * WIDTH, count * WIDTH)], right_side.reshape(count * WIDTH, WIDTH)
        )

    def columns(r, j):
        return pl.ds(pl.multiple_of((r + j) * WIDTH, WIDTH), WIDTH)

    def add_blocks(r, u, count):
        for j in range(3):
            acc[:, columns(r, j)] += product_of(r, u, count, j)

    densify(4)
    for load in load_a:
        load.wait()
    place_a(1, (0,))
    relay(0)
    turn(TURNED[0])
    place_a(1, (1,))
    relay(1)
    turn(TURNED[1])
    for n in range(NB):
        for q in range(3 * CB):
            block = dense[8 + n, :, pl.ds(q * TILE, TILE)]
            p_turned[pl.ds(q * TILE, TILE), pl.ds(n * TILE, TILE)] = block.T
    relay(2)
    place_a(0, (0,))
    relay(3)
    place_a(0, (1,))
    relay(4)
    place_a(2, (0,))
    relay(5)
    place_a(2, (1,))
    densify(3)
    densify(5)
    add_blocks(1, 0, 3)

    for h in range(NCH):
        own_near[h].wait_recv()

    @pl.when(has_l)
    def _():
        for h in range(NCH):
            rel_l_near[h].wait_recv()

    @pl.when(has_r)
    def _():
        for h in range(NCH):
            rel_r_near[h].wait_recv()

    for u in range(3):
        densify(3 * r_near + u)
    add_blocks(r_near, 0, 3)
    for j in range(2):
        at = pl.ds(pl.multiple_of((3 - 3 * core + j) * WIDTH, WIDTH), WIDTH)
        prod[:, at] = acc[:, at].astype(BF16)

    @pl.when(far_ok)
    def _():
        for h in RELAYED:
            own_far[h].wait_recv()

    densify(3 * r_far + 1)
    add_blocks(r_far, 1, 1)

    @pl.when(jnp.logical_and(far_ok, has_l))
    def _():
        for h in RELAYED:
            rel_l_far[h].wait_recv()
        for h in TURNED:
            turn_r[h].wait_recv()

    densify(3 * r_far)

    @pl.when(jnp.logical_and(far_ok, has_r))
    def _():
        for h in RELAYED:
            rel_r_far[h].wait_recv()
        for h in TURNED:
            turn_l[h].wait_recv()

    densify(3 * r_far + 2)
    for j in range(3):
        at = columns(r_far, j)
        prod[:, at] = (acc[:, at] + (product_of(r_far, 0, 1, j) + product_of(r_far, 2, 1, j))).astype(BF16)

    order = [lax.rem(c + off, n_cross) for off in (2, 1, 3, 0)]

    def chunk_of(q, k, at):
        lhs = p_turned[pl.ds(pl.multiple_of(q * WIDTH + order[k] * rows, rows), rows), :]
        return dot(lhs, prod[:, at])

    halves = (pl.ds(0, part_rows), pl.ds(part_rows, part_rows))
    pieces = [(0, b, here) for here in halves for b in range(2)]
    pieces += [(k, b, pl.ds(0, rows)) for k, b in ((1, 1), (2, 0), (1, 0), (2, 1))]
    far_copies = [
        remote(send_far.at[k, b, here], recv_far.at[k, b, here], FAR0 + i, far, c)
        for i, (k, b, here) in enumerate(pieces)
    ]
    far_copies.append(remote(send_far.at[3], recv_far.at[3], FAR0 + 8, far, c))
    near_copies = [remote(send_near.at[k], recv_near.at[k], NEAR0 + k, near, c) for k in range(4)]

    def make_far(k, b):
        send_far[k, b] = chunk_of(r_far, k, pl.ds(b * (PW // 2), PW // 2)).astype(BF16)

    def start_far(*which):
        @pl.when(far_ok)
        def _():
            for i in which:
                far_copies[i].start()

    def send_near_chunk(k):
        for j in range(5):
            at = pl.ds(j * WIDTH, WIDTH)
            send_near[k, :, at] = chunk_of(r_near, k, at).astype(BF16)
        near_copies[k].start()

    def own_chunk(k):
        for j in range(5):
            total[k, :, pl.ds((j + 1) * WIDTH, WIDTH)] = chunk_of(1, k, pl.ds(j * WIDTH, WIDTH))

    make_far(0, 0)
    make_far(0, 1)
    start_far(0, 1, 2, 3)
    send_near_chunk(0)
    make_far(1, 1)
    start_far(4)
    make_far(2, 0)
    start_far(5)
    send_near_chunk(1)
    send_near_chunk(2)
    make_far(1, 0)
    start_far(6)
    make_far(2, 1)
    start_far(7)
    make_far(3, 0)
    make_far(3, 1)
    start_far(8)
    own_chunk(0)
    own_chunk(1)
    own_chunk(2)

    near_at = pl.ds(pl.multiple_of((2 - 2 * core) * WIDTH, WIDTH), PW)
    def add_near(k):
        near_copies[k].wait_recv()
        total[k, :, near_at] += recv_near[k].astype(F32)

    def wait_far(i):
        @pl.when(far_ok)
        def _():
            far_copies[i].wait_recv()

    early_first = pl.multiple_of((5 - 5 * core) * WIDTH, WIDTH)
    late_first = pl.multiple_of(2 * core * WIDTH, WIDTH)
    early = [pl.ds(pl.multiple_of(early_first + i * (EARLY // 2), TILE), EARLY // 2) for i in range(2)]
    late = [pl.ds(pl.multiple_of(late_first + i * (PW // 2), TILE), PW // 2) for i in range(2)]

    to = [right, left]

    def early_copy(step, side):
        i = 2 * step + side
        return remote(e_send.at[i], e_recv.at[i], X0 + i, s, to[side])

    def late_copy(step, side, here, extra):
        i = 2 * step + side
        return remote(x_send.at[i, here], x_recv.at[i, here], X0 + 6 + extra + side, s, to[side])

    e = [[early_copy(step, side) for side in range(2)] for step in range(3)]
    x_two = [[late_copy(0, side, here, 2 * i) for side in range(2)] for i, here in enumerate(halves)]
    x_alone = [late_copy(1, side, pl.ds(0, rows), 4) for side in range(2)]
    x_sum = [[late_copy(2, side, here, 6 + 2 * i) for side in range(2)] for i, here in enumerate(halves)]

    def late_rows(k, b, here):
        return total[k, here, late[b]] + recv_far[k, b, here, :].astype(F32)

    def send_alone(side):
        wait_far(4 + side)
        x_send[2 + side] = late_rows(1 + side, 1 - side, pl.ds(0, rows)).astype(BF16)
        x_alone[side].start()

    add_near(0)
    for side in range(2):
        e_send[side] = total[0, :, early[side]].astype(BF16)
        e[0][side].start()
    for side in range(2):
        add_near(1 + side)
        e_send[2 + side] = total[1 + side, :, early[1 - side]].astype(BF16)
        e[1][side].start()
    for i, here in enumerate(halves):
        for side in range(2):
            wait_far(2 * i + side)
            x_send[side, here, :] = late_rows(0, side, here).astype(BF16)
            x_two[i][side].start()
    send_near_chunk(3)
    own_chunk(3)
    send_alone(0)
    for side in range(2):
        e[0][side].wait_recv()
        e_send[4 + side] = (total[1 + side, :, early[side]] + e_recv[side].astype(F32)).astype(BF16)
        e[2][side].start()
    send_alone(1)
    add_near(3)
    for side in range(2):
        wait_far(6 + side)
        for i, here in enumerate(halves):
            x_two[i][side].wait_recv()
            came = x_recv[side, here, :].astype(F32)
            x_send[4 + side, here, :] = (late_rows(1 + side, side, here) + came).astype(BF16)
            x_sum[i][side].start()
    for side in range(2):
        e[1][side].wait_recv()
        e[2][side].wait_recv()
    for side in range(2):
        out_ref[:, early[side]] = (
            total[3, :, early[side]] + e_recv[4 + side].astype(F32) + e_recv[3 - side].astype(F32)
        )
    wait_far(8)
    for side in range(2):
        x_alone[side].wait_recv()
    for side in range(2):
        total[3, :, late[side]] = late_rows(3, side, pl.ds(0, rows)) + x_recv[3 - side].astype(F32)
    for side in range(2):
        for i, here in enumerate(halves):
            x_sum[i][side].wait_recv()
            out_ref[here, late[side]] = total[3, here, late[side]] + x_recv[4 + side, here, :].astype(F32)

    for copy in list(own_near.values()) + near_copies + e[0] + e[1] + e[2] + x_two[0] + x_two[1] + x_alone + x_sum[0] + x_sum[1]:
        copy.wait_send()

    @pl.when(has_r)
    def _():
        for copy in list(own_r.values()) + list(rel_r_near.values()):
            copy.wait_send()

    @pl.when(has_l)
    def _():
        for copy in list(own_l.values()) + list(rel_l_near.values()):
            copy.wait_send()

    @pl.when(far_ok)
    def _():
        for copy in list(own_far.values()) + far_copies:
            copy.wait_send()

        @pl.when(has_r)
        def _():
            for copy in list(rel_r_far.values()) + list(turn_r.values()):
                copy.wait_send()

        @pl.when(has_l)
        def _():
            for copy in list(rel_l_far.values()) + list(turn_l.values()):
                copy.wait_send()


def body(n_slab, n_cross, a_tiles, a_cols, over_tiles, over_rows, over_cols, p_tiles, p_cols):
    rows = CB * TILE // n_cross
    hbm = pl.BlockSpec(memory_space=pl.ANY)
    return pl.pallas_call(
        functools.partial(kernel, n_slab, n_cross),
        out_shape=pltpu.VMEM((rows, CW), F32),
        in_specs=[hbm] * 7,
        out_specs=pl.BlockSpec(memory_space=pltpu.VMEM),
        scratch_shapes=[
            pltpu.SMEM((NB, K), jnp.int32),
            pltpu.SMEM((OV,), jnp.int32),
            pltpu.SMEM((OV,), jnp.int32),
            pltpu.SMEM((NB, KP), jnp.int32),
            pltpu.VMEM((9, BROWS, TILE), BF16),
            pltpu.VMEM((18, TILE, WIDE), BF16),
            pltpu.VMEM((NB, K + 1, TILE, TILE), BF16),
            pltpu.VMEM((OV + 1, TILE, TILE), BF16),
            pltpu.VMEM((3, NB * TILE, WIDE), BF16),
            pltpu.VMEM((WIDE, NB * TILE), BF16),
            pltpu.VMEM((NB * TILE, PW), F32),
            pltpu.VMEM((NB * TILE, PW), BF16),
            pltpu.VMEM((n_cross, 2, rows, PW // 2), BF16),
            pltpu.VMEM((n_cross, rows, PW), BF16),
            pltpu.VMEM((n_cross, 2, rows, PW // 2), BF16),
            pltpu.VMEM((n_cross, rows, PW), BF16),
            pltpu.VMEM((n_cross, rows, CW), F32),
            pltpu.VMEM((6, rows, EARLY // 2), BF16),
            pltpu.VMEM((6, rows, EARLY // 2), BF16),
            pltpu.VMEM((6, rows, PW // 2), BF16),
            pltpu.VMEM((6, rows, PW // 2), BF16),
            pltpu.SemaphoreType.DMA((7,)),
            pltpu.SemaphoreType.DMA((N_SEMS,)),
            pltpu.SemaphoreType.DMA((N_SEMS,)),
        ],
        compiler_params=pltpu.CompilerParams(collective_id=0, has_side_effects=True),
    )(a_tiles, over_tiles, p_tiles.reshape(NB * KP * TILE, TILE), a_cols, over_rows, over_cols, p_cols)


def solution(mesh):
    return jax.shard_map(
        functools.partial(body, mesh.shape["slab"], mesh.shape["cross"]),
        mesh=mesh,
        in_specs=(
            P(("slab", "cross"), None, None, None),
            P(("slab", "cross"), None),
            P(("slab", "cross"), None, None),
            P(("slab", "cross")),
            P(("slab", "cross")),
            P(("slab", "cross"), None, None, None),
            P(("slab", "cross"), None),
        ),
        out_specs=P(("slab", "cross"), None),
        check_vma=False,
    )
```

```python
import functools

import jax
import jax.numpy as jnp
from jax import lax
from jax.experimental import pallas as pl
from jax.experimental.pallas import tpu as pltpu
from jax.sharding import PartitionSpec as P

CB = 2
TILE = 128
NB = 2
KP = 3
K = 7
OV = 4
WIDTH = CB * TILE
WIDE = 3 * WIDTH
PW = 5 * WIDTH
CW = 7 * WIDTH
EARLY = PW - WIDE
NCH = NB * KP
MARKS = 16
BROWS = MARKS + NCH * TILE
RELAYED = (0, 1, 2, 3)
TURNED = (4, 5)
F32 = jnp.float32
BF16 = jnp.bfloat16

OWN_R, OWN_L, OWN_NEAR, OWN_FAR, REL_L_NEAR, REL_L_FAR, REL_R_NEAR, REL_R_FAR, TURN_R, TURN_L = (
    NCH * i for i in range(10)
)
FAR0 = 10 * NCH
FAR_EARLY = FAR0 + 9
NEAR0 = FAR_EARLY + 4
NEAR_EARLY = NEAR0 + 4
X0 = NEAR_EARLY + 1
N_SEMS = X0 + 22


def dot(a, b):
    return lax.dot_general(a, b, (((1,), (0,)), ((), ())), preferred_element_type=F32)


def kernel(
    n_slab, n_cross,
    a_hbm, o_hbm, p_hbm, a_cols_hbm, over_rows_hbm, over_cols_hbm, p_cols_hbm,
    out_ref,
    a_cols, over_rows, over_cols, p_cols,
    halo, dense, a_in, o_in, a_dense, p_turned, acc, prod,
    early_far, early_near, got_early_far, got_early_near,
    send_far, send_near, recv_far, recv_near, total,
    e_send, e_recv, x_send, x_recv, local_sem, send_sem, recv_sem,
):
    s = lax.axis_index("slab")
    c = lax.axis_index("cross")
    core = lax.rem(s, 2)
    near = s + 1 - 2 * core
    far = s - 1 + 2 * core
    far_ok = jnp.logical_and(far >= 0, far < n_slab)
    right = lax.rem(c + 1, n_cross)
    left = lax.rem(c + n_cross - 1, n_cross)
    has_l = c > 0
    has_r = c < n_cross - 1
    r_near = 2 - 2 * core
    r_far = 2 * core
    rows = CB * TILE // n_cross
    part_rows = rows // 2

    def device(slab, cross):
        return {"slab": slab, "cross": cross}

    def remote(src, dst, i, slab, cross):
        return pltpu.make_async_remote_copy(
            src_ref=src, dst_ref=dst, send_sem=send_sem.at[i], recv_sem=recv_sem.at[i],
            device_id=device(slab, cross), device_id_type=pl.DeviceIdType.MESH,
        )

    barrier = pltpu.get_barrier_semaphore()

    def greet(slab, cross):
        pl.semaphore_signal(
            barrier, inc=1, device_id=device(slab, cross), device_id_type=pl.DeviceIdType.MESH
        )

    @pl.when(far_ok)
    def _():
        greet(far, c)

    greet(s, left)
    greet(s, right)
    greet(near, c)

    load_p = pltpu.make_async_copy(p_hbm, halo.at[4, pl.ds(MARKS, NCH * TILE)], local_sem.at[0])
    load_numbers = pltpu.make_async_copy(p_cols_hbm, p_cols, local_sem.at[1])
    load_a = [
        pltpu.make_async_copy(a_hbm, a_in.at[:, pl.ds(0, K)], local_sem.at[2]),
        pltpu.make_async_copy(a_cols_hbm, a_cols, local_sem.at[3]),
        pltpu.make_async_copy(o_hbm, o_in.at[pl.ds(0, OV)], local_sem.at[4]),
        pltpu.make_async_copy(over_rows_hbm, over_rows, local_sem.at[5]),
        pltpu.make_async_copy(over_cols_hbm, over_cols, local_sem.at[6]),
    ]
    for load in [load_numbers, load_p] + load_a:
        load.start()

    nothing = jnp.full((MARKS, TILE), -1.0, BF16)

    def leave_out(b):
        halo[b, pl.ds(0, MARKS), :] = nothing

    @pl.when(jnp.logical_not(has_l))
    def _():
        for r in range(3):
            leave_out(3 * r)

    @pl.when(jnp.logical_not(has_r))
    def _():
        for r in range(3):
            leave_out(3 * r + 2)

    @pl.when(jnp.logical_not(far_ok))
    def _():
        for u in range(3):
            leave_out(3 * r_far + u)
        recv_far[...] = jnp.zeros_like(recv_far)
        got_early_far[...] = jnp.zeros_like(got_early_far)

    load_numbers.wait()
    row = lax.broadcasted_iota(jnp.int32, (MARKS, TILE), 0)
    value = jnp.full((MARKS, TILE), -1.0, F32)
    for i in range(NCH):
        value = jnp.where(row == i, p_cols[i // KP, i % KP].astype(F32), value)
    halo[4, pl.ds(0, MARKS), :] = value.astype(BF16)
    load_p.wait()
    pl.semaphore_wait(barrier, 3 + far_ok.astype(jnp.int32))

    def halo_copies(b, to, first, slab, cross, chunks=range(NCH)):
        copies = {}
        for h in chunks:
            at = pl.ds(0, MARKS + TILE) if h == 0 else pl.ds(MARKS + h * TILE, TILE)
            copies[h] = remote(halo.at[b, at], halo.at[to, at], first + h, slab, cross)
        return copies

    own_r = halo_copies(4, 3, OWN_R, s, right)
    own_l = halo_copies(4, 5, OWN_L, s, left)
    own_near = halo_copies(4, 3 * r_far + 1, OWN_NEAR, near, c)
    own_far = halo_copies(4, 3 * r_near + 1, OWN_FAR, far, c)
    rel_l_near = halo_copies(3, 3 * r_far, REL_L_NEAR, near, c)
    rel_l_far = halo_copies(3, 3 * r_near, REL_L_FAR, far, c, RELAYED)
    rel_r_near = halo_copies(5, 3 * r_far + 2, REL_R_NEAR, near, c)
    rel_r_far = halo_copies(5, 3 * r_near + 2, REL_R_FAR, far, c, RELAYED)
    turn_r = halo_copies(3 * r_far + 1, 3 * r_far, TURN_R, s, right, TURNED)
    turn_l = halo_copies(3 * r_far + 1, 3 * r_far + 2, TURN_L, s, left, TURNED)

    for h in range(NCH):

        @pl.when(has_r)
        def _():
            own_r[h].start()

        @pl.when(has_l)
        def _():
            own_l[h].start()

    @pl.when(far_ok)
    def _():
        for h in TURNED + RELAYED:
            own_far[h].start()

    for h in range(NCH):
        own_near[h].start()

    for n in range(NB):
        a_in[n, K] = jnp.zeros((TILE, TILE), BF16)
    o_in[OV] = jnp.zeros((TILE, TILE), BF16)
    acc[...] = jnp.zeros_like(acc)
    total[...] = jnp.zeros_like(total)

    def densify(b, places=(0, 1)):
        for n in places:
            tiles, marks = [], []
            numbers = halo[b, pl.ds(0, MARKS), :].astype(F32)
            for i in range(n * KP, n * KP + KP):
                tiles.append(halo[b, pl.ds(MARKS + i * TILE, TILE), :].reshape(8, 16, TILE))
                marks.append(jnp.broadcast_to(numbers[i : i + 1], (16, TILE)).astype(BF16))
            for q in range(3 * CB):
                value = jnp.zeros((8, 16, TILE), BF16)
                for m in range(KP):
                    here = jnp.broadcast_to((marks[m] == jnp.asarray(q, BF16))[None], value.shape)
                    value = jnp.where(here, tiles[m], value)
                dense[2 * b + n, :, pl.ds(q * TILE, TILE)] = value.reshape(TILE, TILE)

    def place_a(r, places=(0, 1)):
        for n in places:
            for t in range(6 * r, 6 * r + 6):
                at = jnp.int32(K)
                for k in range(K):
                    at = jnp.where(a_cols[n, k] == t, k, at)
                value = a_in[n, at].astype(F32)
                for o in range(OV):
                    hit = jnp.logical_and(over_rows[o] == n, over_cols[o] == t)
                    value += o_in[jnp.where(hit, o, OV)].astype(F32)
                a_dense[r, pl.ds(n * TILE, TILE), pl.ds((t % 6) * TILE, TILE)] = value.astype(BF16)

    def relay(h):
        @pl.when(has_l)
        def _():
            own_r[h].wait_recv()
            if h in RELAYED:

                @pl.when(far_ok)
                def _():
                    rel_l_far[h].start()

            rel_l_near[h].start()

        @pl.when(has_r)
        def _():
            own_l[h].wait_recv()
            if h in RELAYED:

                @pl.when(far_ok)
                def _():
                    rel_r_far[h].start()

            rel_r_near[h].start()

    def turn(h):
        @pl.when(far_ok)
        def _():
            own_far[h].wait_recv()

            @pl.when(has_r)
            def _():
                turn_r[h].start()

            @pl.when(has_l)
            def _():
                turn_l[h].start()

    def product_of(r, u, count, j):
        right_side = dense[pl.ds(6 * r + 2 * u, 2 * count), :, pl.ds(j * WIDTH, WIDTH)]
        return dot(
            a_dense[r, :, pl.ds(u * WIDTH, count * WIDTH)], right_side.reshape(count * WIDTH, WIDTH)
        )

    def columns(r, j):
        return pl.ds(pl.multiple_of((r + j) * WIDTH, WIDTH), WIDTH)

    def add_blocks(r, u, count):
        for j in range(3):
            acc[:, columns(r, j)] += product_of(r, u, count, j)

    densify(4)
    for load in load_a:
        load.wait()
    place_a(1, (0,))
    relay(0)
    turn(TURNED[0])
    place_a(1, (1,))
    relay(1)
    turn(TURNED[1])
    for n in range(NB):
        for q in range(3 * CB):
            block = dense[8 + n, :, pl.ds(q * TILE, TILE)]
            p_turned[pl.ds(q * TILE, TILE), pl.ds(n * TILE, TILE)] = block.T
    relay(2)
    place_a(0, (0,))
    relay(3)
    place_a(0, (1,))
    relay(4)
    place_a(2, (0,))
    relay(5)
    place_a(2, (1,))
    densify(3)
    densify(5)
    add_blocks(1, 0, 3)

    for h in range(NCH):
        own_near[h].wait_recv()

    @pl.when(has_l)
    def _():
        for h in range(NCH):
            rel_l_near[h].wait_recv()

    @pl.when(has_r)
    def _():
        for h in range(NCH):
            rel_r_near[h].wait_recv()

    for u in range(3):
        densify(3 * r_near + u)
    add_blocks(r_near, 0, 3)
    order = [lax.rem(c + off, n_cross) for off in (2, 1, 3, 0)]
    early_at = (3 - 3 * core) * WIDTH
    late_at = 2 * core * WIDTH

    def chunk_of(q, k, first, width):
        lhs = p_turned[pl.ds(pl.multiple_of(q * WIDTH + order[k] * rows, rows), rows), :]
        return dot(lhs, prod[:, pl.ds(pl.multiple_of(first, TILE), width)])

    for j in range(2):
        at = pl.ds(pl.multiple_of(early_at + j * WIDTH, WIDTH), WIDTH)
        prod[:, at] = acc[:, at].astype(BF16)

    early_far_copies = [remote(early_far.at[k], got_early_far.at[k], FAR_EARLY + k, far, c) for k in range(4)]
    early_near_copy = remote(early_near, got_early_near, NEAR_EARLY, near, c)
    for k in range(4):
        early_far[k] = chunk_of(r_far, k, early_at, EARLY).astype(BF16)

        @pl.when(far_ok)
        def _():
            early_far_copies[k].start()

    for k in range(4):
        early_near[k] = chunk_of(r_near, k, early_at, EARLY).astype(BF16)
    early_near_copy.start()
    for k in range(4):
        at = pl.ds(pl.multiple_of(early_at + WIDTH, WIDTH), EARLY)
        total[k, :, at] = chunk_of(1, k, early_at, EARLY)

    @pl.when(far_ok)
    def _():
        for h in RELAYED:
            own_far[h].wait_recv()

    densify(3 * r_far + 1)
    add_blocks(r_far, 1, 1)

    first, last = RELAYED[:KP], RELAYED[KP:]
    diagonal = ((0, has_l, rel_l_far, turn_r), (2, has_r, rel_r_far, turn_l))
    for u, has, relayed, turned in diagonal:

        @pl.when(jnp.logical_and(far_ok, has))
        def _():
            for h in first:
                relayed[h].wait_recv()

        densify(3 * r_far + u, (0,))
    for u, has, relayed, turned in diagonal:

        @pl.when(jnp.logical_and(far_ok, has))
        def _():
            for h in last:
                relayed[h].wait_recv()
            for h in TURNED:
                turned[h].wait_recv()

        densify(3 * r_far + u, (1,))
    for j in range(3):
        at = columns(r_far, j)
        prod[:, at] = (acc[:, at] + (product_of(r_far, 0, 1, j) + product_of(r_far, 2, 1, j))).astype(BF16)

    halves = (pl.ds(0, part_rows), pl.ds(part_rows, part_rows))
    every = pl.ds(0, rows)
    pieces = [(0, b, here) for here in halves for b in range(2)]
    pieces += [(k, b, every) for k, b in ((1, 1), (2, 0), (1, 0), (2, 1))]
    far_copies = [
        remote(send_far.at[k, b, here], recv_far.at[k, b, here], FAR0 + i, far, c)
        for i, (k, b, here) in enumerate(pieces)
    ]
    far_copies.append(remote(send_far.at[3], recv_far.at[3], FAR0 + 8, far, c))
    near_copies = [remote(send_near.at[k], recv_near.at[k], NEAR0 + k, near, c) for k in range(4)]

    def make_far(k):
        value = chunk_of(r_far, k, late_at, WIDE).astype(BF16)
        for b in range(2):
            send_far[k, b] = value[:, b * (WIDE // 2) : (b + 1) * (WIDE // 2)]

    def start_far(*which):
        @pl.when(far_ok)
        def _():
            for i in which:
                far_copies[i].start()

    def make_near(k):
        send_near[k] = chunk_of(r_near, k, late_at, WIDE).astype(BF16)
        near_copies[k].start()

    def make_own(k):
        at = pl.ds(pl.multiple_of(late_at + WIDTH, WIDTH), WIDE)
        total[k, :, at] = chunk_of(1, k, late_at, WIDE)

    near_first = 2 * (1 - core) * WIDTH
    near_early = pl.ds(pl.multiple_of(near_first + 3 * core * WIDTH, WIDTH), EARLY)
    near_late = pl.ds(pl.multiple_of(near_first + 2 * (1 - core) * WIDTH, WIDTH), WIDE)

    def add_near(k):
        total[k, :, near_early] += got_early_near[k].astype(F32)
        near_copies[k].wait_recv()
        total[k, :, near_late] += recv_near[k].astype(F32)

    def wait_far(i):
        @pl.when(far_ok)
        def _():
            far_copies[i].wait_recv()

    starts = (5 * core * WIDTH, 5 * (1 - core) * WIDTH, 2 * WIDTH)
    widths = (EARLY // 2, EARLY // 2, WIDE // 2)
    group = [
        [pl.ds(pl.multiple_of(start + b * width, TILE), width) for b in range(2)]
        for start, width in zip(starts, widths)
    ]

    to = [right, left]

    def small_copy(g, step, side):
        i = 6 * g + 2 * step + side
        return remote(e_send.at[i], e_recv.at[i], X0 + i, s, to[side])

    def late_copy(step, side, here, number):
        i = 2 * step + side
        return remote(x_send.at[i, here], x_recv.at[i, here], X0 + 12 + number + side, s, to[side])

    small = [[[small_copy(g, step, side) for side in range(2)] for step in range(3)] for g in range(2)]
    x_two = [[late_copy(0, side, here, 2 * i) for side in range(2)] for i, here in enumerate(halves)]
    x_alone = [late_copy(1, side, every, 4) for side in range(2)]
    x_sum = [[late_copy(2, side, here, 6 + 2 * i) for side in range(2)] for i, here in enumerate(halves)]

    def small_rows(g, k, b):
        value = total[k, :, group[g][b]]
        if g == 0:
            value += got_early_far[k, :, b * widths[0] : (b + 1) * widths[0]].astype(F32)
        return value

    def send_small(g, step, side):
        k = (0, 1 + side, 1 + side)[step]
        b = (side, 1 - side, side)[step]
        value = small_rows(g, k, b)
        if step == 2:
            small[g][0][side].wait_recv()
            value += e_recv[6 * g + side].astype(F32)
        e_send[6 * g + 2 * step + side] = value.astype(BF16)
        small[g][step][side].start()

    def late_rows(k, b, here):
        return total[k, here, group[2][b]] + recv_far[k, b, here, :].astype(F32)

    def send_alone(side):
        wait_far(4 + side)
        x_send[2 + side] = late_rows(1 + side, 1 - side, every).astype(BF16)
        x_alone[side].start()

    make_far(0)
    start_far(0, 1, 2, 3)
    make_own(0)

    @pl.when(far_ok)
    def _():
        for copy in early_far_copies:
            copy.wait_recv()

    for side in range(2):
        send_small(0, 0, side)
    make_near(0)
    for k in (1, 2):
        make_far(k)
        start_far(3 + k)
        make_own(k)
        send_small(0, 1, k - 1)
        make_near(k)
    start_far(6, 7)
    early_near_copy.wait_recv()
    add_near(0)
    for side in range(2):
        send_small(1, 0, side)
    for side in range(2):
        add_near(1 + side)
        send_small(1, 1, side)
    make_far(3)
    start_far(8)
    for i, here in enumerate(halves):
        for side in range(2):
            wait_far(2 * i + side)
            x_send[side, here, :] = late_rows(0, side, here).astype(BF16)
            x_two[i][side].start()
    make_near(3)
    make_own(3)
    for side in range(2):
        send_small(0, 2, side)
    for side in range(2):
        send_alone(side)
    for side in range(2):
        send_small(1, 2, side)
    for side in range(2):
        wait_far(6 + side)
    for i, here in enumerate(halves):
        for side in range(2):
            x_two[i][side].wait_recv()
            came = x_recv[side, here, :].astype(F32)
            x_send[4 + side, here, :] = (late_rows(1 + side, side, here) + came).astype(BF16)
            x_sum[i][side].start()
    add_near(3)
    for g in range(2):
        for step in (1, 2):
            for side in range(2):
                small[g][step][side].wait_recv()
        for side in range(2):
            out_ref[:, group[g][side]] = (
                small_rows(g, 3, side) + e_recv[6 * g + 4 + side].astype(F32) + e_recv[6 * g + 3 - side].astype(F32)
            )
    wait_far(8)
    for side in range(2):
        x_alone[side].wait_recv()
    for side in range(2):
        total[3, :, group[2][side]] = late_rows(3, side, every) + x_recv[3 - side].astype(F32)
    for i, here in enumerate(halves):
        for side in range(2):
            x_sum[i][side].wait_recv()
            out_ref[here, group[2][side]] = total[3, here, group[2][side]] + x_recv[4 + side, here, :].astype(F32)

    sums = [copy for steps in small for sides in steps for copy in sides]
    sums += x_two[0] + x_two[1] + x_alone + x_sum[0] + x_sum[1]
    for copy in list(own_near.values()) + [early_near_copy] + near_copies + sums:
        copy.wait_send()

    @pl.when(has_r)
    def _():
        for copy in list(own_r.values()) + list(rel_r_near.values()):
            copy.wait_send()

    @pl.when(has_l)
    def _():
        for copy in list(own_l.values()) + list(rel_l_near.values()):
            copy.wait_send()

    @pl.when(far_ok)
    def _():
        for copy in list(own_far.values()) + early_far_copies + far_copies:
            copy.wait_send()

        @pl.when(has_r)
        def _():
            for copy in list(rel_r_far.values()) + list(turn_r.values()):
                copy.wait_send()

        @pl.when(has_l)
        def _():
            for copy in list(rel_l_far.values()) + list(turn_l.values()):
                copy.wait_send()


def body(n_slab, n_cross, a_tiles, a_cols, over_tiles, over_rows, over_cols, p_tiles, p_cols):
    rows = CB * TILE // n_cross
    hbm = pl.BlockSpec(memory_space=pl.ANY)
    return pl.pallas_call(
        functools.partial(kernel, n_slab, n_cross),
        out_shape=pltpu.VMEM((rows, CW), F32),
        in_specs=[hbm] * 7,
        out_specs=pl.BlockSpec(memory_space=pltpu.VMEM),
        scratch_shapes=[
            pltpu.SMEM((NB, K), jnp.int32),
            pltpu.SMEM((OV,), jnp.int32),
            pltpu.SMEM((OV,), jnp.int32),
            pltpu.SMEM((NB, KP), jnp.int32),
            pltpu.VMEM((9, BROWS, TILE), BF16),
            pltpu.VMEM((18, TILE, WIDE), BF16),
            pltpu.VMEM((NB, K + 1, TILE, TILE), BF16),
            pltpu.VMEM((OV + 1, TILE, TILE), BF16),
            pltpu.VMEM((3, NB * TILE, WIDE), BF16),
            pltpu.VMEM((WIDE, NB * TILE), BF16),
            pltpu.VMEM((NB * TILE, PW), F32),
            pltpu.VMEM((NB * TILE, PW), BF16),
            pltpu.VMEM((n_cross, rows, EARLY), BF16),
            pltpu.VMEM((n_cross, rows, EARLY), BF16),
            pltpu.VMEM((n_cross, rows, EARLY), BF16),
            pltpu.VMEM((n_cross, rows, EARLY), BF16),
            pltpu.VMEM((n_cross, 2, rows, WIDE // 2), BF16),
            pltpu.VMEM((n_cross, rows, WIDE), BF16),
            pltpu.VMEM((n_cross, 2, rows, WIDE // 2), BF16),
            pltpu.VMEM((n_cross, rows, WIDE), BF16),
            pltpu.VMEM((n_cross, rows, CW), F32),
            pltpu.VMEM((12, rows, EARLY // 2), BF16),
            pltpu.VMEM((12, rows, EARLY // 2), BF16),
            pltpu.VMEM((6, rows, WIDE // 2), BF16),
            pltpu.VMEM((6, rows, WIDE // 2), BF16),
            pltpu.SemaphoreType.DMA((7,)),
            pltpu.SemaphoreType.DMA((N_SEMS,)),
            pltpu.SemaphoreType.DMA((N_SEMS,)),
        ],
        compiler_params=pltpu.CompilerParams(collective_id=0, has_side_effects=True),
    )(a_tiles, over_tiles, p_tiles.reshape(NB * KP * TILE, TILE), a_cols, over_rows, over_cols, p_cols)


def solution(mesh):
    return jax.shard_map(
        functools.partial(body, mesh.shape["slab"], mesh.shape["cross"]),
        mesh=mesh,
        in_specs=(
            P(("slab", "cross"), None, None, None),
            P(("slab", "cross"), None),
            P(("slab", "cross"), None, None),
            P(("slab", "cross")),
            P(("slab", "cross")),
            P(("slab", "cross"), None, None, None),
            P(("slab", "cross"), None),
        ),
        out_specs=P(("slab", "cross"), None),
        check_vma=False,
    )
```

```python
import functools

import jax
import jax.numpy as jnp
from jax import lax
from jax.experimental import pallas as pl
from jax.experimental.pallas import tpu as pltpu
from jax.sharding import PartitionSpec as P

CB = 2
TILE = 128
NB = 2
KP = 3
K = 7
OV = 4
WIDTH = CB * TILE
WIDE = 3 * WIDTH
PW = 5 * WIDTH
CW = 7 * WIDTH
EARLY = CW - PW
NCH = NB * KP
MARKS = 16
BROWS = MARKS + NCH * TILE
RELAYED = (0, 1, 2, 3)
TURNED = (4, 5)
F32 = jnp.float32
BF16 = jnp.bfloat16

OWN_R, OWN_L, OWN_NEAR, OWN_FAR, REL_L_NEAR, REL_L_FAR, REL_R_NEAR, REL_R_FAR, TURN_R, TURN_L = (
    NCH * i for i in range(10)
)
FAR0 = 10 * NCH
BESIDE = FAR0 + 7
NEAR0 = BESIDE + 2
X0 = NEAR0 + 4
N_SEMS = X0 + 16


def dot(a, b):
    return lax.dot_general(a, b, (((1,), (0,)), ((), ())), preferred_element_type=F32)


def kernel(
    n_slab, n_cross,
    a_hbm, o_hbm, p_hbm, a_cols_hbm, over_rows_hbm, over_cols_hbm, p_cols_hbm,
    out_ref,
    a_cols, over_rows, over_cols, p_cols,
    halo, dense, a_in, o_in, a_dense, p_turned, acc, prod,
    send_far, send_near, recv_far, recv_near, last_far, beside, total,
    e_send, e_recv, x_send, x_recv, local_sem, send_sem, recv_sem,
):
    s = lax.axis_index("slab")
    c = lax.axis_index("cross")
    core = lax.rem(s, 2)
    near = s + 1 - 2 * core
    far = s - 1 + 2 * core
    far_ok = jnp.logical_and(far >= 0, far < n_slab)
    right = lax.rem(c + 1, n_cross)
    left = lax.rem(c + n_cross - 1, n_cross)
    has_l = c > 0
    has_r = c < n_cross - 1
    r_near = 2 - 2 * core
    r_far = 2 * core
    rows = CB * TILE // n_cross
    part_rows = rows // 2

    def device(slab, cross):
        return {"slab": slab, "cross": cross}

    def remote(src, dst, i, slab, cross):
        return pltpu.make_async_remote_copy(
            src_ref=src, dst_ref=dst, send_sem=send_sem.at[i], recv_sem=recv_sem.at[i],
            device_id=device(slab, cross), device_id_type=pl.DeviceIdType.MESH,
        )

    barrier = pltpu.get_barrier_semaphore()

    def greet(slab, cross):
        pl.semaphore_signal(
            barrier, inc=1, device_id=device(slab, cross), device_id_type=pl.DeviceIdType.MESH
        )

    @pl.when(far_ok)
    def _():
        greet(far, c)

    greet(s, left)
    greet(s, right)
    greet(near, c)

    load_p = pltpu.make_async_copy(p_hbm, halo.at[4, pl.ds(MARKS, NCH * TILE)], local_sem.at[0])
    load_numbers = pltpu.make_async_copy(p_cols_hbm, p_cols, local_sem.at[1])
    load_a = [
        pltpu.make_async_copy(a_hbm, a_in.at[:, pl.ds(0, K)], local_sem.at[2]),
        pltpu.make_async_copy(a_cols_hbm, a_cols, local_sem.at[3]),
        pltpu.make_async_copy(o_hbm, o_in.at[pl.ds(0, OV)], local_sem.at[4]),
        pltpu.make_async_copy(over_rows_hbm, over_rows, local_sem.at[5]),
        pltpu.make_async_copy(over_cols_hbm, over_cols, local_sem.at[6]),
    ]
    for load in [load_numbers, load_p] + load_a:
        load.start()

    nothing = jnp.full((MARKS, TILE), -1.0, BF16)

    def leave_out(b):
        halo[b, pl.ds(0, MARKS), :] = nothing

    @pl.when(jnp.logical_not(has_l))
    def _():
        for r in range(3):
            leave_out(3 * r)

    @pl.when(jnp.logical_not(has_r))
    def _():
        for r in range(3):
            leave_out(3 * r + 2)

    @pl.when(jnp.logical_not(far_ok))
    def _():
        for u in range(3):
            leave_out(3 * r_far + u)
        recv_far[...] = jnp.zeros_like(recv_far)

    load_numbers.wait()
    row = lax.broadcasted_iota(jnp.int32, (MARKS, TILE), 0)
    value = jnp.full((MARKS, TILE), -1.0, F32)
    for i in range(NCH):
        value = jnp.where(row == i, p_cols[i // KP, i % KP].astype(F32), value)
    halo[4, pl.ds(0, MARKS), :] = value.astype(BF16)
    load_p.wait()
    pl.semaphore_wait(barrier, 3 + far_ok.astype(jnp.int32))

    def halo_copies(b, to, first, slab, cross, chunks=range(NCH)):
        copies = {}
        for h in chunks:
            at = pl.ds(0, MARKS + TILE) if h == 0 else pl.ds(MARKS + h * TILE, TILE)
            copies[h] = remote(halo.at[b, at], halo.at[to, at], first + h, slab, cross)
        return copies

    own_r = halo_copies(4, 3, OWN_R, s, right)
    own_l = halo_copies(4, 5, OWN_L, s, left)
    own_near = halo_copies(4, 3 * r_far + 1, OWN_NEAR, near, c)
    own_far = halo_copies(4, 3 * r_near + 1, OWN_FAR, far, c)
    rel_l_near = halo_copies(3, 3 * r_far, REL_L_NEAR, near, c)
    rel_l_far = halo_copies(3, 3 * r_near, REL_L_FAR, far, c, RELAYED)
    rel_r_near = halo_copies(5, 3 * r_far + 2, REL_R_NEAR, near, c)
    rel_r_far = halo_copies(5, 3 * r_near + 2, REL_R_FAR, far, c, RELAYED)
    turn_r = halo_copies(3 * r_far + 1, 3 * r_far, TURN_R, s, right, TURNED)
    turn_l = halo_copies(3 * r_far + 1, 3 * r_far + 2, TURN_L, s, left, TURNED)

    for h in range(NCH):

        @pl.when(has_r)
        def _():
            own_r[h].start()

        @pl.when(has_l)
        def _():
            own_l[h].start()

    @pl.when(far_ok)
    def _():
        for h in TURNED + RELAYED:
            own_far[h].start()

    for h in range(NCH):
        own_near[h].start()

    for n in range(NB):
        a_in[n, K] = jnp.zeros((TILE, TILE), BF16)
    o_in[OV] = jnp.zeros((TILE, TILE), BF16)
    acc[...] = jnp.zeros_like(acc)
    total[...] = jnp.zeros_like(total)

    def densify(b, places=(0, 1)):
        for n in places:
            tiles, marks = [], []
            numbers = halo[b, pl.ds(0, MARKS), :].astype(F32)
            for i in range(n * KP, n * KP + KP):
                tiles.append(halo[b, pl.ds(MARKS + i * TILE, TILE), :].reshape(8, 16, TILE))
                marks.append(jnp.broadcast_to(numbers[i : i + 1], (16, TILE)).astype(BF16))
            for q in range(3 * CB):
                value = jnp.zeros((8, 16, TILE), BF16)
                for m in range(KP):
                    here = jnp.broadcast_to((marks[m] == jnp.asarray(q, BF16))[None], value.shape)
                    value = jnp.where(here, tiles[m], value)
                dense[2 * b + n, :, pl.ds(q * TILE, TILE)] = value.reshape(TILE, TILE)

    def place_a(r, places=(0, 1)):
        for n in places:
            for t in range(6 * r, 6 * r + 6):
                at = jnp.int32(K)
                for k in range(K):
                    at = jnp.where(a_cols[n, k] == t, k, at)
                value = a_in[n, at].astype(F32)
                for o in range(OV):
                    hit = jnp.logical_and(over_rows[o] == n, over_cols[o] == t)
                    value += o_in[jnp.where(hit, o, OV)].astype(F32)
                a_dense[r, pl.ds(n * TILE, TILE), pl.ds((t % 6) * TILE, TILE)] = value.astype(BF16)

    def relay(h):
        @pl.when(has_l)
        def _():
            own_r[h].wait_recv()
            if h in RELAYED:

                @pl.when(far_ok)
                def _():
                    rel_l_far[h].start()

            rel_l_near[h].start()

        @pl.when(has_r)
        def _():
            own_l[h].wait_recv()
            if h in RELAYED:

                @pl.when(far_ok)
                def _():
                    rel_r_far[h].start()

            rel_r_near[h].start()

    def turn(h):
        @pl.when(far_ok)
        def _():
            own_far[h].wait_recv()

            @pl.when(has_r)
            def _():
                turn_r[h].start()

            @pl.when(has_l)
            def _():
                turn_l[h].start()

    def product_of(r, u, count, j):
        right_side = dense[pl.ds(6 * r + 2 * u, 2 * count), :, pl.ds(j * WIDTH, WIDTH)]
        return dot(
            a_dense[r, :, pl.ds(u * WIDTH, count * WIDTH)], right_side.reshape(count * WIDTH, WIDTH)
        )

    def columns(r, j):
        return pl.ds(pl.multiple_of((r + j) * WIDTH, WIDTH), WIDTH)

    def add_own(r):
        densify(3 * r + 1)
        for j in range(3):
            acc[:, columns(r, j)] += product_of(r, 1, 1, j)

    def add_sides(r):
        for j in range(3):
            acc[:, columns(r, j)] += product_of(r, 0, 1, j) + product_of(r, 2, 1, j)

    near_sides = ((0, has_l, rel_l_near), (2, has_r, rel_r_near))
    far_sides = ((0, has_l, rel_l_far, turn_r), (2, has_r, rel_r_far, turn_l))
    first, rest = range(KP), range(KP, NCH)

    def near_rows(n):
        for u, has, relayed in near_sides:

            @pl.when(has)
            def _():
                for h in (first, rest)[n]:
                    relayed[h].wait_recv()

            densify(3 * r_near + u, (n,))

    def far_rows(n):
        for u, has, relayed, turned in far_sides:

            @pl.when(jnp.logical_and(far_ok, has))
            def _():
                for h in (first, rest)[n]:
                    (relayed if h in RELAYED else turned)[h].wait_recv()

            densify(3 * r_far + u, (n,))

    for load in load_a:
        load.wait()
    place_a(1)
    relay(0)
    turn(TURNED[0])
    add_own(1)
    relay(1)
    turn(TURNED[1])
    for n in range(NB):
        for q in range(3 * CB):
            block = dense[8 + n, :, pl.ds(q * TILE, TILE)]
            p_turned[pl.ds(q * TILE, TILE), pl.ds(n * TILE, TILE)] = block.T
    place_a(0)
    relay(2)
    place_a(2)
    relay(3)
    densify(3, (0,))
    densify(5, (0,))
    for h in range(NCH):
        own_near[h].wait_recv()
    add_own(r_near)
    relay(4)
    near_rows(0)

    @pl.when(far_ok)
    def _():
        for h in RELAYED:
            own_far[h].wait_recv()

    relay(5)
    add_own(r_far)
    densify(3, (1,))
    densify(5, (1,))
    add_sides(1)
    near_rows(1)
    add_sides(r_near)
    for j in range(2):
        at = pl.ds(pl.multiple_of((3 - 3 * core + j) * WIDTH, WIDTH), WIDTH)
        prod[:, at] = acc[:, at].astype(BF16)

    far_rows(0)
    far_rows(1)
    for j in range(3):
        at = columns(r_far, j)
        prod[:, at] = (acc[:, at] + (product_of(r_far, 0, 1, j) + product_of(r_far, 2, 1, j))).astype(BF16)

    order = [lax.rem(c + off, n_cross) for off in (2, 1, 3, 0)]

    def chunk_of(q, k, at):
        lhs = p_turned[pl.ds(pl.multiple_of(q * WIDTH + order[k] * rows, rows), rows), :]
        return dot(lhs, prod[:, at])

    halves = (pl.ds(0, part_rows), pl.ds(part_rows, part_rows))
    pieces = [(0, b, here) for here in halves for b in range(2)]
    pieces += [(k, b, pl.ds(0, rows)) for k, b in ((1, 0), (2, 1))]
    far_copies = [
        remote(send_far.at[k, b, here], recv_far.at[k, b, here], FAR0 + i, far, c)
        for i, (k, b, here) in enumerate(pieces)
    ]
    far_copies.append(remote(send_far.at[3], recv_far.at[3], FAR0 + 6, far, c))
    beside_copies = [
        remote(send_far.at[1 + side, 1 - side], beside.at[1 - side], BESIDE + side, s, (right, left)[side])
        for side in range(2)
    ]
    near_copies = [remote(send_near.at[k], recv_near.at[k], NEAR0 + k, near, c) for k in range(4)]

    def make_far(k, b):
        send_far[k, b] = chunk_of(r_far, k, pl.ds(b * (PW // 2), PW // 2)).astype(BF16)

    def start_far(*which):
        @pl.when(far_ok)
        def _():
            for i in which:
                far_copies[i].start()

    def send_near_chunk(k):
        for j in range(5):
            at = pl.ds(j * WIDTH, WIDTH)
            send_near[k, :, at] = chunk_of(r_near, k, at).astype(BF16)
        near_copies[k].start()

    def own_chunk(k):
        for j in range(5):
            total[k, :, pl.ds((j + 1) * WIDTH, WIDTH)] = chunk_of(1, k, pl.ds(j * WIDTH, WIDTH))

    make_far(0, 0)
    make_far(0, 1)
    start_far(0, 1, 2, 3)
    for side in range(2):
        make_far(1 + side, 1 - side)

        @pl.when(far_ok)
        def _():
            beside_copies[side].start()

    send_near_chunk(0)
    for side in range(2):
        make_far(1 + side, side)
        start_far(4 + side)
    send_near_chunk(1)
    send_near_chunk(2)
    own_chunk(0)
    own_chunk(1)
    own_chunk(2)

    near_at = pl.ds(pl.multiple_of((2 - 2 * core) * WIDTH, WIDTH), PW)
    def add_near(k):
        near_copies[k].wait_recv()
        total[k, :, near_at] += recv_near[k].astype(F32)

    def wait_far(i):
        @pl.when(far_ok)
        def _():
            far_copies[i].wait_recv()

    early_first = pl.multiple_of((5 - 5 * core) * WIDTH, WIDTH)
    late_first = pl.multiple_of(2 * core * WIDTH, WIDTH)
    early = [pl.ds(pl.multiple_of(early_first + i * (EARLY // 2), TILE), EARLY // 2) for i in range(2)]
    late = [pl.ds(pl.multiple_of(late_first + i * (PW // 2), TILE), PW // 2) for i in range(2)]

    to = [right, left]

    def early_copy(step, side):
        i = 2 * step + side
        return remote(e_send.at[i], e_recv.at[i], X0 + i, s, to[side])

    def late_copy(step, side, here, extra):
        i = 2 * step + side
        return remote(x_send.at[i, here], x_recv.at[i, here], X0 + 6 + extra + side, s, to[side])

    e = [[early_copy(step, side) for side in range(2)] for step in range(3)]
    x_two = [[late_copy(0, side, here, 2 * i) for side in range(2)] for i, here in enumerate(halves)]
    x_alone = [late_copy(1, side, pl.ds(0, rows), 4) for side in range(2)]
    x_sum = [[late_copy(2, side, here, 6 + 2 * i) for side in range(2)] for i, here in enumerate(halves)]

    def late_rows(k, b, here):
        return total[k, here, late[b]] + recv_far[k, b, here, :].astype(F32)

    def send_alone(side):
        x_send[2 + side] = total[1 + side, :, late[1 - side]].astype(BF16)
        x_alone[side].start()

    add_near(0)
    for side in range(2):
        e_send[side] = total[0, :, early[side]].astype(BF16)
        e[0][side].start()
    for side in range(2):
        add_near(1 + side)
        e_send[2 + side] = total[1 + side, :, early[1 - side]].astype(BF16)
        e[1][side].start()
    for b in range(2):
        last_far[b] = chunk_of(r_far, 3, pl.ds(b * (PW // 2), PW // 2))
    for i, here in enumerate(halves):
        for side in range(2):
            wait_far(2 * i + side)
            x_send[side, here, :] = late_rows(0, side, here).astype(BF16)
            x_two[i][side].start()

    @pl.when(far_ok)
    def _():
        for b in range(2):
            beside_copies[1 - b].wait_recv()
            send_far[3, b] = (last_far[b] + beside[b].astype(F32)).astype(BF16)

    start_far(6)
    for side in range(2):
        send_alone(side)
    for side in range(2):
        e[0][side].wait_recv()
        e_send[4 + side] = (total[1 + side, :, early[side]] + e_recv[side].astype(F32)).astype(BF16)
        e[2][side].start()
    send_near_chunk(3)
    own_chunk(3)
    for side in range(2):
        wait_far(4 + side)
    for i, here in enumerate(halves):
        for side in range(2):
            x_two[i][side].wait_recv()
            came = x_recv[side, here, :].astype(F32)
            x_send[4 + side, here, :] = (late_rows(1 + side, side, here) + came).astype(BF16)
            x_sum[i][side].start()
    add_near(3)
    for side in range(2):
        e[1][side].wait_recv()
        e[2][side].wait_recv()
    for side in range(2):
        out_ref[:, early[side]] = (
            total[3, :, early[side]] + e_recv[4 + side].astype(F32) + e_recv[3 - side].astype(F32)
        )
    wait_far(6)
    for side in range(2):
        x_alone[side].wait_recv()
    for side in range(2):
        total[3, :, late[side]] = late_rows(3, side, pl.ds(0, rows)) + x_recv[3 - side].astype(F32)
    for i, here in enumerate(halves):
        for side in range(2):
            x_sum[i][side].wait_recv()
            out_ref[here, late[side]] = total[3, here, late[side]] + x_recv[4 + side, here, :].astype(F32)

    for copy in list(own_near.values()) + near_copies + e[0] + e[1] + e[2] + x_two[0] + x_two[1] + x_alone + x_sum[0] + x_sum[1]:
        copy.wait_send()

    @pl.when(has_r)
    def _():
        for copy in list(own_r.values()) + list(rel_r_near.values()):
            copy.wait_send()

    @pl.when(has_l)
    def _():
        for copy in list(own_l.values()) + list(rel_l_near.values()):
            copy.wait_send()

    @pl.when(far_ok)
    def _():
        for copy in list(own_far.values()) + far_copies + beside_copies:
            copy.wait_send()

        @pl.when(has_r)
        def _():
            for copy in list(rel_r_far.values()) + list(turn_r.values()):
                copy.wait_send()

        @pl.when(has_l)
        def _():
            for copy in list(rel_l_far.values()) + list(turn_l.values()):
                copy.wait_send()


def body(n_slab, n_cross, a_tiles, a_cols, over_tiles, over_rows, over_cols, p_tiles, p_cols):
    rows = CB * TILE // n_cross
    hbm = pl.BlockSpec(memory_space=pl.ANY)
    return pl.pallas_call(
        functools.partial(kernel, n_slab, n_cross),
        out_shape=pltpu.VMEM((rows, CW), F32),
        in_specs=[hbm] * 7,
        out_specs=pl.BlockSpec(memory_space=pltpu.VMEM),
        scratch_shapes=[
            pltpu.SMEM((NB, K), jnp.int32),
            pltpu.SMEM((OV,), jnp.int32),
            pltpu.SMEM((OV,), jnp.int32),
            pltpu.SMEM((NB, KP), jnp.int32),
            pltpu.VMEM((9, BROWS, TILE), BF16),
            pltpu.VMEM((18, TILE, WIDE), BF16),
            pltpu.VMEM((NB, K + 1, TILE, TILE), BF16),
            pltpu.VMEM((OV + 1, TILE, TILE), BF16),
            pltpu.VMEM((3, NB * TILE, WIDE), BF16),
            pltpu.VMEM((WIDE, NB * TILE), BF16),
            pltpu.VMEM((NB * TILE, PW), F32),
            pltpu.VMEM((NB * TILE, PW), BF16),
            pltpu.VMEM((n_cross, 2, rows, PW // 2), BF16),
            pltpu.VMEM((n_cross, rows, PW), BF16),
            pltpu.VMEM((n_cross, 2, rows, PW // 2), BF16),
            pltpu.VMEM((n_cross, rows, PW), BF16),
            pltpu.VMEM((2, rows, PW // 2), F32),
            pltpu.VMEM((2, rows, PW // 2), BF16),
            pltpu.VMEM((n_cross, rows, CW), F32),
            pltpu.VMEM((6, rows, EARLY // 2), BF16),
            pltpu.VMEM((6, rows, EARLY // 2), BF16),
            pltpu.VMEM((6, rows, PW // 2), BF16),
            pltpu.VMEM((6, rows, PW // 2), BF16),
            pltpu.SemaphoreType.DMA((7,)),
            pltpu.SemaphoreType.DMA((N_SEMS,)),
            pltpu.SemaphoreType.DMA((N_SEMS,)),
        ],
        compiler_params=pltpu.CompilerParams(collective_id=0, has_side_effects=True),
    )(a_tiles, over_tiles, p_tiles.reshape(NB * KP * TILE, TILE), a_cols, over_rows, over_cols, p_cols)


def solution(mesh):
    return jax.shard_map(
        functools.partial(body, mesh.shape["slab"], mesh.shape["cross"]),
        mesh=mesh,
        in_specs=(
            P(("slab", "cross"), None, None, None),
            P(("slab", "cross"), None),
            P(("slab", "cross"), None, None),
            P(("slab", "cross")),
            P(("slab", "cross")),
            P(("slab", "cross"), None, None, None),
            P(("slab", "cross"), None),
        ),
        out_specs=P(("slab", "cross"), None),
        check_vma=False,
    )
```

```python
import functools

import jax
import jax.numpy as jnp
from jax import lax
from jax.experimental import pallas as pl
from jax.experimental.pallas import tpu as pltpu
from jax.sharding import PartitionSpec as P

CB = 2
TILE = 128
NB = 2
KP = 3
K = 7
OV = 4
WIDTH = CB * TILE
WIDE = 3 * WIDTH
PW = 5 * WIDTH
CW = 7 * WIDTH
EARLY = CW - PW
NCH = NB * KP
MARKS = 16
BROWS = MARKS + NCH * TILE
RELAYED = (0, 1, 2, 3)
TURNED = (4, 5)
RUN = 16
CUTS = 4
F32 = jnp.float32
BF16 = jnp.bfloat16

OWN_R, OWN_L, OWN_NEAR, OWN_FAR, REL_L_NEAR, REL_L_FAR, REL_R_NEAR, REL_R_FAR, TURN_R, TURN_L = (
    NCH * i for i in range(10)
)
FAR0 = 10 * NCH
BESIDE = FAR0 + 2 * CUTS + 3
NEAR0 = BESIDE + 2
X0 = NEAR0 + 4
N_SEMS = X0 + 8 + 4 * CUTS


def dot(a, b):
    return lax.dot_general(a, b, (((1,), (0,)), ((), ())), preferred_element_type=F32)


def kernel(
    n_slab, n_cross,
    a_hbm, o_hbm, p_hbm, a_cols_hbm, over_rows_hbm, over_cols_hbm, p_cols_hbm,
    out_ref,
    a_cols, over_rows, over_cols, p_cols,
    halo, dense, a_in, o_in, a_dense, p_turned, acc, prod,
    send_far, send_near, recv_far, recv_near, last_far, beside, total,
    e_send, e_recv, x_send, x_recv, local_sem, send_sem, recv_sem,
):
    s = lax.axis_index("slab")
    c = lax.axis_index("cross")
    core = lax.rem(s, 2)
    near = s + 1 - 2 * core
    far = s - 1 + 2 * core
    far_ok = jnp.logical_and(far >= 0, far < n_slab)
    begins = lax.rem(s, RUN) == 0
    ends = lax.rem(s, RUN) == RUN - 1
    relays_far = jnp.logical_and(far_ok, jnp.logical_not(ends))
    right = lax.rem(c + 1, n_cross)
    left = lax.rem(c + n_cross - 1, n_cross)
    has_l = c > 0
    has_r = c < n_cross - 1
    r_near = 2 - 2 * core
    r_far = 2 * core
    rows = CB * TILE // n_cross
    part_rows = rows // CUTS

    def device(slab, cross):
        return {"slab": slab, "cross": cross}

    def remote(src, dst, i, slab, cross):
        return pltpu.make_async_remote_copy(
            src_ref=src, dst_ref=dst, send_sem=send_sem.at[i], recv_sem=recv_sem.at[i],
            device_id=device(slab, cross), device_id_type=pl.DeviceIdType.MESH,
        )

    barrier = pltpu.get_barrier_semaphore()

    def greet(slab, cross):
        pl.semaphore_signal(
            barrier, inc=1, device_id=device(slab, cross), device_id_type=pl.DeviceIdType.MESH
        )

    @pl.when(far_ok)
    def _():
        greet(far, c)

    greet(s, left)
    greet(s, right)
    greet(near, c)

    load_p = pltpu.make_async_copy(p_hbm, halo.at[4, pl.ds(MARKS, NCH * TILE)], local_sem.at[0])
    load_numbers = pltpu.make_async_copy(p_cols_hbm, p_cols, local_sem.at[1])
    load_a = [
        pltpu.make_async_copy(a_hbm, a_in.at[:, pl.ds(0, K)], local_sem.at[2]),
        pltpu.make_async_copy(a_cols_hbm, a_cols, local_sem.at[3]),
        pltpu.make_async_copy(o_hbm, o_in.at[pl.ds(0, OV)], local_sem.at[4]),
        pltpu.make_async_copy(over_rows_hbm, over_rows, local_sem.at[5]),
        pltpu.make_async_copy(over_cols_hbm, over_cols, local_sem.at[6]),
    ]
    for load in [load_numbers, load_p] + load_a:
        load.start()

    nothing = jnp.full((MARKS, TILE), -1.0, BF16)

    def leave_out(b):
        halo[b, pl.ds(0, MARKS), :] = nothing

    @pl.when(jnp.logical_not(has_l))
    def _():
        for r in range(3):
            leave_out(3 * r)

    @pl.when(jnp.logical_not(has_r))
    def _():
        for r in range(3):
            leave_out(3 * r + 2)

    @pl.when(jnp.logical_not(far_ok))
    def _():
        for u in range(3):
            leave_out(3 * r_far + u)
        recv_far[...] = jnp.zeros_like(recv_far)

    load_numbers.wait()
    row = lax.broadcasted_iota(jnp.int32, (MARKS, TILE), 0)
    value = jnp.full((MARKS, TILE), -1.0, F32)
    for i in range(NCH):
        value = jnp.where(row == i, p_cols[i // KP, i % KP].astype(F32), value)
    halo[4, pl.ds(0, MARKS), :] = value.astype(BF16)
    load_p.wait()
    pl.semaphore_wait(barrier, 3 + far_ok.astype(jnp.int32))

    def halo_copies(b, to, first, slab, cross, chunks=range(NCH)):
        copies = {}
        for h in chunks:
            at = pl.ds(0, MARKS + TILE) if h == 0 else pl.ds(MARKS + h * TILE, TILE)
            copies[h] = remote(halo.at[b, at], halo.at[to, at], first + h, slab, cross)
        return copies

    own_r = halo_copies(4, 3, OWN_R, s, right)
    own_l = halo_copies(4, 5, OWN_L, s, left)
    own_near = halo_copies(4, 3 * r_far + 1, OWN_NEAR, near, c)
    own_far = halo_copies(4, 3 * r_near + 1, OWN_FAR, far, c)
    rel_l_near = halo_copies(3, 3 * r_far, REL_L_NEAR, near, c)
    rel_l_far = halo_copies(3, 3 * r_near, REL_L_FAR, far, c, RELAYED)
    rel_r_near = halo_copies(5, 3 * r_far + 2, REL_R_NEAR, near, c)
    rel_r_far = halo_copies(5, 3 * r_near + 2, REL_R_FAR, far, c, RELAYED)
    turn_r = halo_copies(3 * r_far + 1, 3 * r_far, TURN_R, s, right)
    turn_l = halo_copies(3 * r_far + 1, 3 * r_far + 2, TURN_L, s, left)

    for h in range(NCH):

        @pl.when(has_r)
        def _():
            own_r[h].start()

        @pl.when(has_l)
        def _():
            own_l[h].start()

    @pl.when(far_ok)
    def _():
        for h in TURNED + RELAYED:
            own_far[h].start()

    for h in range(NCH):
        own_near[h].start()

    for n in range(NB):
        a_in[n, K] = jnp.zeros((TILE, TILE), BF16)
    o_in[OV] = jnp.zeros((TILE, TILE), BF16)
    acc[...] = jnp.zeros_like(acc)
    total[...] = jnp.zeros_like(total)

    def densify(b, places=(0, 1)):
        for n in places:
            tiles, marks = [], []
            numbers = halo[b, pl.ds(0, MARKS), :].astype(F32)
            for i in range(n * KP, n * KP + KP):
                tiles.append(halo[b, pl.ds(MARKS + i * TILE, TILE), :].reshape(8, 16, TILE))
                marks.append(jnp.broadcast_to(numbers[i : i + 1], (16, TILE)).astype(BF16))
            for q in range(3 * CB):
                value = jnp.zeros((8, 16, TILE), BF16)
                for m in range(KP):
                    here = jnp.broadcast_to((marks[m] == jnp.asarray(q, BF16))[None], value.shape)
                    value = jnp.where(here, tiles[m], value)
                dense[2 * b + n, :, pl.ds(q * TILE, TILE)] = value.reshape(TILE, TILE)

    def place_a(r, places=(0, 1)):
        for n in places:
            for t in range(6 * r, 6 * r + 6):
                at = jnp.int32(K)
                for k in range(K):
                    at = jnp.where(a_cols[n, k] == t, k, at)
                value = a_in[n, at].astype(F32)
                for o in range(OV):
                    hit = jnp.logical_and(over_rows[o] == n, over_cols[o] == t)
                    value += o_in[jnp.where(hit, o, OV)].astype(F32)
                a_dense[r, pl.ds(n * TILE, TILE), pl.ds((t % 6) * TILE, TILE)] = value.astype(BF16)

    def relay(h):
        @pl.when(has_l)
        def _():
            own_r[h].wait_recv()
            if h in RELAYED:

                @pl.when(relays_far)
                def _():
                    rel_l_far[h].start()

            rel_l_near[h].start()

        @pl.when(has_r)
        def _():
            own_l[h].wait_recv()
            if h in RELAYED:

                @pl.when(relays_far)
                def _():
                    rel_r_far[h].start()

            rel_r_near[h].start()

    def turn(h):
        own_far[h].wait_recv()

        @pl.when(has_r)
        def _():
            turn_r[h].start()

        @pl.when(has_l)
        def _():
            turn_l[h].start()

    def turn_unless_late(h):
        @pl.when(jnp.logical_and(far_ok, jnp.logical_not(begins)))
        def _():
            turn(h)

    def product_of(r, u, count, j):
        right_side = dense[pl.ds(6 * r + 2 * u, 2 * count), :, pl.ds(j * WIDTH, WIDTH)]
        return dot(
            a_dense[r, :, pl.ds(u * WIDTH, count * WIDTH)], right_side.reshape(count * WIDTH, WIDTH)
        )

    def columns(r, j):
        return pl.ds(pl.multiple_of((r + j) * WIDTH, WIDTH), WIDTH)

    def add_own(r):
        densify(3 * r + 1)
        for j in range(3):
            acc[:, columns(r, j)] += product_of(r, 1, 1, j)

    def add_sides(r):
        for j in range(3):
            acc[:, columns(r, j)] += product_of(r, 0, 1, j) + product_of(r, 2, 1, j)

    near_sides = ((0, has_l, rel_l_near), (2, has_r, rel_r_near))
    far_sides = ((0, has_l, rel_l_far, turn_r), (2, has_r, rel_r_far, turn_l))
    first, rest = range(KP), range(KP, NCH)

    def near_rows(n):
        for u, has, relayed in near_sides:

            @pl.when(has)
            def _():
                for h in (first, rest)[n]:
                    relayed[h].wait_recv()

            densify(3 * r_near + u, (n,))

    def far_rows(n):
        for u, has, relayed, turned in far_sides:

            for h in (first, rest)[n]:
                comes = jnp.logical_and(far_ok, has)
                if h in RELAYED:

                    @pl.when(jnp.logical_and(comes, jnp.logical_not(begins)))
                    def _():
                        relayed[h].wait_recv()

                    comes = jnp.logical_and(comes, begins)

                @pl.when(comes)
                def _():
                    turned[h].wait_recv()

            densify(3 * r_far + u, (n,))

    for load in load_a:
        load.wait()
    place_a(1)
    relay(0)
    turn_unless_late(TURNED[0])
    add_own(1)
    relay(1)
    turn_unless_late(TURNED[1])
    for n in range(NB):
        for q in range(3 * CB):
            block = dense[8 + n, :, pl.ds(q * TILE, TILE)]
            p_turned[pl.ds(q * TILE, TILE), pl.ds(n * TILE, TILE)] = block.T
    place_a(0)
    relay(2)
    place_a(2)
    relay(3)
    densify(3, (0,))
    densify(5, (0,))
    for h in range(NCH):
        own_near[h].wait_recv()
    add_own(r_near)
    relay(4)
    near_rows(0)
    relay(5)

    @pl.when(jnp.logical_and(far_ok, begins))
    def _():
        for h in TURNED + RELAYED:
            turn(h)

    @pl.when(jnp.logical_and(far_ok, jnp.logical_not(begins)))
    def _():
        for h in RELAYED:
            own_far[h].wait_recv()

    add_own(r_far)
    densify(3, (1,))
    densify(5, (1,))
    add_sides(1)
    near_rows(1)
    add_sides(r_near)
    for j in range(2):
        at = pl.ds(pl.multiple_of((3 - 3 * core + j) * WIDTH, WIDTH), WIDTH)
        prod[:, at] = acc[:, at].astype(BF16)

    far_rows(0)
    far_rows(1)
    for j in range(3):
        at = columns(r_far, j)
        prod[:, at] = (acc[:, at] + (product_of(r_far, 0, 1, j) + product_of(r_far, 2, 1, j))).astype(BF16)

    order = [lax.rem(c + off, n_cross) for off in (2, 1, 3, 0)]

    def chunk_of(q, k, at):
        lhs = p_turned[pl.ds(pl.multiple_of(q * WIDTH + order[k] * rows, rows), rows), :]
        return dot(lhs, prod[:, at])

    halves = [pl.ds(i * part_rows, part_rows) for i in range(CUTS)]
    pieces = [(0, b, here) for here in halves for b in range(2)]
    pieces += [(k, b, pl.ds(0, rows)) for k, b in ((1, 0), (2, 1))]
    far_copies = [
        remote(send_far.at[k, b, here], recv_far.at[k, b, here], FAR0 + i, far, c)
        for i, (k, b, here) in enumerate(pieces)
    ]
    far_copies.append(remote(send_far.at[3], recv_far.at[3], FAR0 + 2 * CUTS + 2, far, c))
    beside_copies = [
        remote(send_far.at[1 + side, 1 - side], beside.at[1 - side], BESIDE + side, s, (right, left)[side])
        for side in range(2)
    ]
    near_copies = [remote(send_near.at[k], recv_near.at[k], NEAR0 + k, near, c) for k in range(4)]

    def make_far(k, b):
        send_far[k, b] = chunk_of(r_far, k, pl.ds(b * (PW // 2), PW // 2)).astype(BF16)

    def start_far(*which):
        @pl.when(far_ok)
        def _():
            for i in which:
                far_copies[i].start()

    def send_near_chunk(k):
        for j in range(5):
            at = pl.ds(j * WIDTH, WIDTH)
            send_near[k, :, at] = chunk_of(r_near, k, at).astype(BF16)
        near_copies[k].start()

    def own_chunk(k):
        for j in range(5):
            total[k, :, pl.ds((j + 1) * WIDTH, WIDTH)] = chunk_of(1, k, pl.ds(j * WIDTH, WIDTH))

    make_far(0, 0)
    make_far(0, 1)
    start_far(*range(2 * CUTS))
    for side in range(2):
        make_far(1 + side, 1 - side)

        @pl.when(far_ok)
        def _():
            beside_copies[side].start()

    send_near_chunk(0)
    for side in range(2):
        make_far(1 + side, side)
        start_far(2 * CUTS + side)
    send_near_chunk(1)
    send_near_chunk(2)
    own_chunk(0)
    own_chunk(1)
    own_chunk(2)

    near_at = pl.ds(pl.multiple_of((2 - 2 * core) * WIDTH, WIDTH), PW)
    def add_near(k):
        near_copies[k].wait_recv()
        total[k, :, near_at] += recv_near[k].astype(F32)

    def wait_far(i):
        @pl.when(far_ok)
        def _():
            far_copies[i].wait_recv()

    early_first = pl.multiple_of((5 - 5 * core) * WIDTH, WIDTH)
    late_first = pl.multiple_of(2 * core * WIDTH, WIDTH)
    early = [pl.ds(pl.multiple_of(early_first + i * (EARLY // 2), TILE), EARLY // 2) for i in range(2)]
    late = [pl.ds(pl.multiple_of(late_first + i * (PW // 2), TILE), PW // 2) for i in range(2)]

    to = [right, left]

    def early_copy(step, side):
        i = 2 * step + side
        return remote(e_send.at[i], e_recv.at[i], X0 + i, s, to[side])

    def late_copy(step, side, here, extra):
        i = 2 * step + side
        return remote(x_send.at[i, here], x_recv.at[i, here], X0 + 6 + extra + side, s, to[side])

    e = [[early_copy(step, side) for side in range(2)] for step in range(3)]
    x_two = [[late_copy(0, side, here, 2 * i) for side in range(2)] for i, here in enumerate(halves)]
    x_alone = [late_copy(1, side, pl.ds(0, rows), 2 * CUTS) for side in range(2)]
    x_sum = [[late_copy(2, side, here, 2 * CUTS + 2 + 2 * i) for side in range(2)] for i, here in enumerate(halves)]

    def late_rows(k, b, here):
        return total[k, here, late[b]] + recv_far[k, b, here, :].astype(F32)

    def send_alone(side):
        x_send[2 + side] = total[1 + side, :, late[1 - side]].astype(BF16)
        x_alone[side].start()

    add_near(0)
    for side in range(2):
        e_send[side] = total[0, :, early[side]].astype(BF16)
        e[0][side].start()
    for side in range(2):
        add_near(1 + side)
        e_send[2 + side] = total[1 + side, :, early[1 - side]].astype(BF16)
        e[1][side].start()
    for b in range(2):
        last_far[b] = chunk_of(r_far, 3, pl.ds(b * (PW // 2), PW // 2))
    for i, here in enumerate(halves):
        for side in range(2):
            wait_far(2 * i + side)
            x_send[side, here, :] = late_rows(0, side, here).astype(BF16)
            x_two[i][side].start()

    @pl.when(far_ok)
    def _():
        for b in range(2):
            beside_copies[1 - b].wait_recv()
            send_far[3, b] = (last_far[b] + beside[b].astype(F32)).astype(BF16)

    start_far(2 * CUTS + 2)
    for side in range(2):
        send_alone(side)
    for side in range(2):
        e[0][side].wait_recv()
        e_send[4 + side] = (total[1 + side, :, early[side]] + e_recv[side].astype(F32)).astype(BF16)
        e[2][side].start()
    send_near_chunk(3)
    own_chunk(3)
    for side in range(2):
        wait_far(2 * CUTS + side)
    for i, here in enumerate(halves):
        for side in range(2):
            x_two[i][side].wait_recv()
            came = x_recv[side, here, :].astype(F32)
            x_send[4 + side, here, :] = (late_rows(1 + side, side, here) + came).astype(BF16)
            x_sum[i][side].start()
    add_near(3)
    for side in range(2):
        e[1][side].wait_recv()
        e[2][side].wait_recv()
    for side in range(2):
        out_ref[:, early[side]] = (
            total[3, :, early[side]] + e_recv[4 + side].astype(F32) + e_recv[3 - side].astype(F32)
        )
    wait_far(2 * CUTS + 2)
    for side in range(2):
        x_alone[side].wait_recv()
    for side in range(2):
        total[3, :, late[side]] = late_rows(3, side, pl.ds(0, rows)) + x_recv[3 - side].astype(F32)
    for i, here in enumerate(halves):
        for side in range(2):
            x_sum[i][side].wait_recv()
            out_ref[here, late[side]] = total[3, here, late[side]] + x_recv[4 + side, here, :].astype(F32)

    for copy in list(own_near.values()) + near_copies + e[0] + e[1] + e[2] + sum(x_two + x_sum, x_alone):
        copy.wait_send()

    @pl.when(has_r)
    def _():
        for copy in list(own_r.values()) + list(rel_r_near.values()):
            copy.wait_send()

    @pl.when(has_l)
    def _():
        for copy in list(own_l.values()) + list(rel_l_near.values()):
            copy.wait_send()

    @pl.when(far_ok)
    def _():
        for copy in list(own_far.values()) + far_copies + beside_copies:
            copy.wait_send()

        for has, relayed, turned in ((has_r, rel_r_far, turn_r), (has_l, rel_l_far, turn_l)):

            @pl.when(jnp.logical_and(has, relays_far))
            def _():
                for h in RELAYED:
                    relayed[h].wait_send()

            @pl.when(has)
            def _():
                for h in TURNED:
                    turned[h].wait_send()

            @pl.when(jnp.logical_and(has, begins))
            def _():
                for h in RELAYED:
                    turned[h].wait_send()


def body(n_slab, n_cross, a_tiles, a_cols, over_tiles, over_rows, over_cols, p_tiles, p_cols):
    rows = CB * TILE // n_cross
    hbm = pl.BlockSpec(memory_space=pl.ANY)
    return pl.pallas_call(
        functools.partial(kernel, n_slab, n_cross),
        out_shape=pltpu.VMEM((rows, CW), F32),
        in_specs=[hbm] * 7,
        out_specs=pl.BlockSpec(memory_space=pltpu.VMEM),
        scratch_shapes=[
            pltpu.SMEM((NB, K), jnp.int32),
            pltpu.SMEM((OV,), jnp.int32),
            pltpu.SMEM((OV,), jnp.int32),
            pltpu.SMEM((NB, KP), jnp.int32),
            pltpu.VMEM((9, BROWS, TILE), BF16),
            pltpu.VMEM((18, TILE, WIDE), BF16),
            pltpu.VMEM((NB, K + 1, TILE, TILE), BF16),
            pltpu.VMEM((OV + 1, TILE, TILE), BF16),
            pltpu.VMEM((3, NB * TILE, WIDE), BF16),
            pltpu.VMEM((WIDE, NB * TILE), BF16),
            pltpu.VMEM((NB * TILE, PW), F32),
            pltpu.VMEM((NB * TILE, PW), BF16),
            pltpu.VMEM((n_cross, 2, rows, PW // 2), BF16),
            pltpu.VMEM((n_cross, rows, PW), BF16),
            pltpu.VMEM((n_cross, 2, rows, PW // 2), BF16),
            pltpu.VMEM((n_cross, rows, PW), BF16),
            pltpu.VMEM((2, rows, PW // 2), F32),
            pltpu.VMEM((2, rows, PW // 2), BF16),
            pltpu.VMEM((n_cross, rows, CW), F32),
            pltpu.VMEM((6, rows, EARLY // 2), BF16),
            pltpu.VMEM((6, rows, EARLY // 2), BF16),
            pltpu.VMEM((6, rows, PW // 2), BF16),
            pltpu.VMEM((6, rows, PW // 2), BF16),
            pltpu.SemaphoreType.DMA((7,)),
            pltpu.SemaphoreType.DMA((N_SEMS,)),
            pltpu.SemaphoreType.DMA((N_SEMS,)),
        ],
        compiler_params=pltpu.CompilerParams(collective_id=0, has_side_effects=True),
    )(a_tiles, over_tiles, p_tiles.reshape(NB * KP * TILE, TILE), a_cols, over_rows, over_cols, p_cols)


def solution(mesh):
    return jax.shard_map(
        functools.partial(body, mesh.shape["slab"], mesh.shape["cross"]),
        mesh=mesh,
        in_specs=(
            P(("slab", "cross"), None, None, None),
            P(("slab", "cross"), None),
            P(("slab", "cross"), None, None),
            P(("slab", "cross")),
            P(("slab", "cross")),
            P(("slab", "cross"), None, None, None),
            P(("slab", "cross"), None),
        ),
        out_specs=P(("slab", "cross"), None),
        check_vma=False,
    )
```

```python
import functools

import jax
import jax.numpy as jnp
from jax import lax
from jax.experimental import pallas as pl
from jax.experimental.pallas import tpu as pltpu
from jax.sharding import PartitionSpec as P

CB = 2
TILE = 128
NB = 2
KP = 3
K = 7
OV = 4
WIDTH = CB * TILE
WIDE = 3 * WIDTH
PW = 5 * WIDTH
CW = 7 * WIDTH
EARLY = CW - PW
NCH = NB * KP
MARKS = 16
BROWS = MARKS + NCH * TILE
RELAYED = (0, 1, 2, 3)
TURNED = (4, 5)
TO_ENDS = (0, 1)
RUN = 16
CUTS = 2
F32 = jnp.float32
BF16 = jnp.bfloat16

OWN_R, OWN_L, OWN_NEAR, OWN_FAR, REL_L_NEAR, REL_L_FAR, REL_R_NEAR, REL_R_FAR, TURN_R, TURN_L = (
    NCH * i for i in range(10)
)
FAR0 = 10 * NCH
BESIDE = FAR0 + 2 * CUTS + 3
NEAR0 = BESIDE + 2
X0 = NEAR0 + 4
N_SEMS = X0 + 8 + 4 * CUTS


def dot(a, b):
    return lax.dot_general(a, b, (((1,), (0,)), ((), ())), preferred_element_type=F32)


def kernel(
    n_slab, n_cross,
    a_hbm, o_hbm, p_hbm, a_cols_hbm, over_rows_hbm, over_cols_hbm, p_cols_hbm,
    out_ref,
    a_cols, over_rows, over_cols, p_cols,
    halo, dense, a_in, o_in, a_dense, p_turned, acc, prod,
    send_far, send_near, recv_far, recv_near, last_far, beside, total,
    e_send, e_recv, x_send, x_recv, far_in, local_sem, send_sem, recv_sem,
):
    s = lax.axis_index("slab")
    c = lax.axis_index("cross")
    core = lax.rem(s, 2)
    near = s + 1 - 2 * core
    far = s - 1 + 2 * core
    far_ok = jnp.logical_and(far >= 0, far < n_slab)
    begins = lax.rem(s, RUN) == 0
    ends = lax.rem(s, RUN) == RUN - 1
    inside = jnp.logical_not(jnp.logical_or(begins, ends))
    far_inside = jnp.logical_and(far_ok, inside)
    far_begins = jnp.logical_and(far_ok, begins)
    far_ends = jnp.logical_and(far_ok, ends)
    right = lax.rem(c + 1, n_cross)
    left = lax.rem(c + n_cross - 1, n_cross)
    has_l = c > 0
    has_r = c < n_cross - 1
    r_near = 2 - 2 * core
    r_far = 2 * core
    rows = CB * TILE // n_cross
    part_rows = rows // CUTS

    def device(slab, cross):
        return {"slab": slab, "cross": cross}

    def remote(src, dst, i, slab, cross):
        return pltpu.make_async_remote_copy(
            src_ref=src, dst_ref=dst, send_sem=send_sem.at[i], recv_sem=recv_sem.at[i],
            device_id=device(slab, cross), device_id_type=pl.DeviceIdType.MESH,
        )

    barrier = pltpu.get_barrier_semaphore()

    def greet(slab, cross):
        pl.semaphore_signal(
            barrier, inc=1, device_id=device(slab, cross), device_id_type=pl.DeviceIdType.MESH
        )

    @pl.when(jnp.logical_and(far_ok, jnp.logical_not(ends)))
    def _():
        greet(far, c)

    greet(s, left)
    greet(s, right)
    greet(near, c)

    load_p = pltpu.make_async_copy(p_hbm, halo.at[4, pl.ds(MARKS, NCH * TILE)], local_sem.at[0])
    load_numbers = pltpu.make_async_copy(p_cols_hbm, p_cols, local_sem.at[1])
    load_a = [
        pltpu.make_async_copy(a_hbm, a_in.at[:, pl.ds(0, K)], local_sem.at[2]),
        pltpu.make_async_copy(a_cols_hbm, a_cols, local_sem.at[3]),
        pltpu.make_async_copy(o_hbm, o_in.at[pl.ds(0, OV)], local_sem.at[4]),
        pltpu.make_async_copy(over_rows_hbm, over_rows, local_sem.at[5]),
        pltpu.make_async_copy(over_cols_hbm, over_cols, local_sem.at[6]),
    ]
    for load in [load_numbers, load_p] + load_a:
        load.start()

    nothing = jnp.full((MARKS, TILE), -1.0, BF16)

    def leave_out(b):
        halo[b, pl.ds(0, MARKS), :] = nothing

    @pl.when(jnp.logical_not(has_l))
    def _():
        for r in range(3):
            leave_out(3 * r)

    @pl.when(jnp.logical_not(has_r))
    def _():
        for r in range(3):
            leave_out(3 * r + 2)

    @pl.when(jnp.logical_not(far_ok))
    def _():
        for u in range(3):
            leave_out(3 * r_far + u)
        recv_far[...] = jnp.zeros_like(recv_far)

    load_numbers.wait()
    row = lax.broadcasted_iota(jnp.int32, (MARKS, TILE), 0)
    value = jnp.full((MARKS, TILE), -1.0, F32)
    for i in range(NCH):
        value = jnp.where(row == i, p_cols[i // KP, i % KP].astype(F32), value)
    halo[4, pl.ds(0, MARKS), :] = value.astype(BF16)
    load_p.wait()
    pl.semaphore_wait(barrier, 3 + jnp.logical_and(far_ok, jnp.logical_not(begins)).astype(jnp.int32))

    @pl.when(far_ends)
    def _():
        pl.semaphore_signal(far_in, inc=1, device_id=device(far, c), device_id_type=pl.DeviceIdType.MESH)

    def halo_copies(b, to, first, slab, cross, chunks=range(NCH)):
        copies = {}
        for h in chunks:
            at = pl.ds(0, MARKS + TILE) if h == 0 else pl.ds(MARKS + h * TILE, TILE)
            copies[h] = remote(halo.at[b, at], halo.at[to, at], first + h, slab, cross)
        return copies

    own_r = halo_copies(4, 3, OWN_R, s, right)
    own_l = halo_copies(4, 5, OWN_L, s, left)
    own_near = halo_copies(4, 3 * r_far + 1, OWN_NEAR, near, c)
    own_far = halo_copies(4, 3 * r_near + 1, OWN_FAR, far, c)
    rel_l_near = halo_copies(3, 3 * r_far, REL_L_NEAR, near, c)
    rel_l_far = halo_copies(3, 3 * r_near, REL_L_FAR, far, c, RELAYED)
    rel_r_near = halo_copies(5, 3 * r_far + 2, REL_R_NEAR, near, c)
    rel_r_far = halo_copies(5, 3 * r_near + 2, REL_R_FAR, far, c, RELAYED)
    turn_r = halo_copies(3 * r_far + 1, 3 * r_far, TURN_R, s, right)
    turn_l = halo_copies(3 * r_far + 1, 3 * r_far + 2, TURN_L, s, left)

    for h in range(NCH):

        @pl.when(has_r)
        def _():
            own_r[h].start()

        @pl.when(has_l)
        def _():
            own_l[h].start()

    @pl.when(jnp.logical_and(far_ok, jnp.logical_not(begins)))
    def _():
        for h in TURNED + RELAYED:
            own_far[h].start()

    for h in range(NCH):
        own_near[h].start()

    for n in range(NB):
        a_in[n, K] = jnp.zeros((TILE, TILE), BF16)
    o_in[OV] = jnp.zeros((TILE, TILE), BF16)
    acc[...] = jnp.zeros_like(acc)
    total[...] = jnp.zeros_like(total)

    def densify(b, places=(0, 1)):
        for n in places:
            tiles, marks = [], []
            numbers = halo[b, pl.ds(0, MARKS), :].astype(F32)
            for i in range(n * KP, n * KP + KP):
                tiles.append(halo[b, pl.ds(MARKS + i * TILE, TILE), :].reshape(8, 16, TILE))
                marks.append(jnp.broadcast_to(numbers[i : i + 1], (16, TILE)).astype(BF16))
            for q in range(3 * CB):
                value = jnp.zeros((8, 16, TILE), BF16)
                for m in range(KP):
                    here = jnp.broadcast_to((marks[m] == jnp.asarray(q, BF16))[None], value.shape)
                    value = jnp.where(here, tiles[m], value)
                dense[2 * b + n, :, pl.ds(q * TILE, TILE)] = value.reshape(TILE, TILE)

    def place_a(r, places=(0, 1)):
        for n in places:
            for t in range(6 * r, 6 * r + 6):
                at = jnp.int32(K)
                for k in range(K):
                    at = jnp.where(a_cols[n, k] == t, k, at)
                value = a_in[n, at].astype(F32)
                for o in range(OV):
                    hit = jnp.logical_and(over_rows[o] == n, over_cols[o] == t)
                    value += o_in[jnp.where(hit, o, OV)].astype(F32)
                a_dense[r, pl.ds(n * TILE, TILE), pl.ds((t % 6) * TILE, TILE)] = value.astype(BF16)

    def relay(h):
        @pl.when(has_l)
        def _():
            own_r[h].wait_recv()
            if h in RELAYED:

                @pl.when(far_inside)
                def _():
                    rel_l_far[h].start()

            rel_l_near[h].start()

        @pl.when(has_r)
        def _():
            own_l[h].wait_recv()
            if h in RELAYED:

                @pl.when(far_inside)
                def _():
                    rel_r_far[h].start()

            rel_r_near[h].start()

    def turn(h):
        own_far[h].wait_recv()

        @pl.when(has_r)
        def _():
            turn_r[h].start()

        @pl.when(has_l)
        def _():
            turn_l[h].start()

    def turn_inside(h):
        @pl.when(far_inside)
        def _():
            turn(h)

    def product_of(r, u, count, j):
        right_side = dense[pl.ds(6 * r + 2 * u, 2 * count), :, pl.ds(j * WIDTH, WIDTH)]
        return dot(
            a_dense[r, :, pl.ds(u * WIDTH, count * WIDTH)], right_side.reshape(count * WIDTH, WIDTH)
        )

    def columns(r, j):
        return pl.ds(pl.multiple_of((r + j) * WIDTH, WIDTH), WIDTH)

    def add_own(r):
        densify(3 * r + 1)
        for j in range(3):
            acc[:, columns(r, j)] += product_of(r, 1, 1, j)

    def add_sides(r):
        for j in range(3):
            acc[:, columns(r, j)] += product_of(r, 0, 1, j) + product_of(r, 2, 1, j)

    near_sides = ((0, has_l, rel_l_near), (2, has_r, rel_r_near))
    far_sides = ((0, has_l, rel_l_far, turn_r), (2, has_r, rel_r_far, turn_l))
    first, rest = range(KP), range(KP, NCH)

    def near_rows(n):
        for u, has, relayed in near_sides:

            @pl.when(has)
            def _():
                for h in (first, rest)[n]:
                    relayed[h].wait_recv()

            densify(3 * r_near + u, (n,))

    def turned_here(h):
        return begins if h in TO_ENDS else jnp.logical_or(begins, ends)

    def far_rows(n):
        for u, has, relayed, turned in far_sides:

            for h in (first, rest)[n]:
                comes = jnp.logical_and(far_ok, has)
                if h in RELAYED:
                    over_slab_first = turned_here(h)

                    @pl.when(jnp.logical_and(comes, jnp.logical_not(over_slab_first)))
                    def _():
                        relayed[h].wait_recv()

                    comes = jnp.logical_and(comes, over_slab_first)

                @pl.when(comes)
                def _():
                    turned[h].wait_recv()

            densify(3 * r_far + u, (n,))

    for load in load_a:
        load.wait()
    place_a(1)
    relay(0)
    turn_inside(TURNED[0])
    add_own(1)
    relay(1)
    turn_inside(TURNED[1])
    for n in range(NB):
        for q in range(3 * CB):
            block = dense[8 + n, :, pl.ds(q * TILE, TILE)]
            p_turned[pl.ds(q * TILE, TILE), pl.ds(n * TILE, TILE)] = block.T
    place_a(0)
    relay(2)
    place_a(2)
    relay(3)
    densify(3, (0,))
    densify(5, (0,))
    for h in range(NCH):
        own_near[h].wait_recv()
    add_own(r_near)
    relay(4)
    near_rows(0)
    relay(5)

    beyond = [h for h in range(NCH) if h not in TO_ENDS]

    @pl.when(far_begins)
    def _():
        pl.semaphore_wait(far_in, 1)
        for h in beyond:
            own_far[h].start()
        for h in TO_ENDS:
            own_far[h].start()
        for h in TO_ENDS:

            @pl.when(has_l)
            def _():
                rel_l_far[h].start()

            @pl.when(has_r)
            def _():
                rel_r_far[h].start()

        for h in TURNED + RELAYED:
            turn(h)

    @pl.when(far_ends)
    def _():
        for h in beyond:
            turn(h)
        for h in TO_ENDS:
            own_far[h].wait_recv()

    @pl.when(far_inside)
    def _():
        for h in RELAYED:
            own_far[h].wait_recv()

    add_own(r_far)
    densify(3, (1,))
    densify(5, (1,))
    add_sides(1)
    near_rows(1)
    add_sides(r_near)
    for j in range(2):
        at = pl.ds(pl.multiple_of((3 - 3 * core + j) * WIDTH, WIDTH), WIDTH)
        prod[:, at] = acc[:, at].astype(BF16)

    far_rows(0)
    far_rows(1)
    for j in range(3):
        at = columns(r_far, j)
        prod[:, at] = (acc[:, at] + (product_of(r_far, 0, 1, j) + product_of(r_far, 2, 1, j))).astype(BF16)

    order = [lax.rem(c + off, n_cross) for off in (2, 1, 3, 0)]

    def chunk_of(q, k, at):
        lhs = p_turned[pl.ds(pl.multiple_of(q * WIDTH + order[k] * rows, rows), rows), :]
        return dot(lhs, prod[:, at])

    halves = [pl.ds(i * part_rows, part_rows) for i in range(CUTS)]
    pieces = [(0, b, here) for here in halves for b in range(2)]
    pieces += [(k, b, pl.ds(0, rows)) for k, b in ((1, 0), (2, 1))]
    far_copies = [
        remote(send_far.at[k, b, here], recv_far.at[k, b, here], FAR0 + i, far, c)
        for i, (k, b, here) in enumerate(pieces)
    ]
    far_copies.append(remote(send_far.at[3], recv_far.at[3], FAR0 + 2 * CUTS + 2, far, c))
    beside_copies = [
        remote(send_far.at[1 + side, 1 - side], beside.at[1 - side], BESIDE + side, s, (right, left)[side])
        for side in range(2)
    ]
    near_copies = [remote(send_near.at[k], recv_near.at[k], NEAR0 + k, near, c) for k in range(4)]

    def make_far(k, b):
        send_far[k, b] = chunk_of(r_far, k, pl.ds(b * (PW // 2), PW // 2)).astype(BF16)

    def start_far(*which):
        @pl.when(far_ok)
        def _():
            for i in which:
                far_copies[i].start()

    def send_near_chunk(k):
        for j in range(5):
            at = pl.ds(j * WIDTH, WIDTH)
            send_near[k, :, at] = chunk_of(r_near, k, at).astype(BF16)
        near_copies[k].start()

    def own_chunk(k):
        for j in range(5):
            total[k, :, pl.ds((j + 1) * WIDTH, WIDTH)] = chunk_of(1, k, pl.ds(j * WIDTH, WIDTH))

    make_far(0, 0)
    make_far(0, 1)
    start_far(*range(2 * CUTS))
    for side in range(2):
        make_far(1 + side, 1 - side)

        @pl.when(far_ok)
        def _():
            beside_copies[side].start()

    send_near_chunk(0)
    for side in range(2):
        make_far(1 + side, side)
        start_far(2 * CUTS + side)
    send_near_chunk(1)
    send_near_chunk(2)
    own_chunk(0)
    own_chunk(1)
    own_chunk(2)

    near_at = pl.ds(pl.multiple_of((2 - 2 * core) * WIDTH, WIDTH), PW)
    def add_near(k):
        near_copies[k].wait_recv()
        total[k, :, near_at] += recv_near[k].astype(F32)

    def wait_far(i):
        @pl.when(far_ok)
        def _():
            far_copies[i].wait_recv()

    early_first = pl.multiple_of((5 - 5 * core) * WIDTH, WIDTH)
    late_first = pl.multiple_of(2 * core * WIDTH, WIDTH)
    early = [pl.ds(pl.multiple_of(early_first + i * (EARLY // 2), TILE), EARLY // 2) for i in range(2)]
    late = [pl.ds(pl.multiple_of(late_first + i * (PW // 2), TILE), PW // 2) for i in range(2)]

    to = [right, left]

    def early_copy(step, side):
        i = 2 * step + side
        return remote(e_send.at[i], e_recv.at[i], X0 + i, s, to[side])

    def late_copy(step, side, here, extra):
        i = 2 * step + side
        return remote(x_send.at[i, here], x_recv.at[i, here], X0 + 6 + extra + side, s, to[side])

    e = [[early_copy(step, side) for side in range(2)] for step in range(3)]
    x_two = [[late_copy(0, side, here, 2 * i) for side in range(2)] for i, here in enumerate(halves)]
    x_alone = [late_copy(1, side, pl.ds(0, rows), 2 * CUTS) for side in range(2)]
    x_sum = [[late_copy(2, side, here, 2 * CUTS + 2 + 2 * i) for side in range(2)] for i, here in enumerate(halves)]

    def late_rows(k, b, here):
        return total[k, here, late[b]] + recv_far[k, b, here, :].astype(F32)

    def send_alone(side):
        x_send[2 + side] = total[1 + side, :, late[1 - side]].astype(BF16)
        x_alone[side].start()

    add_near(0)
    for side in range(2):
        e_send[side] = total[0, :, early[side]].astype(BF16)
        e[0][side].start()
    for side in range(2):
        add_near(1 + side)
        e_send[2 + side] = total[1 + side, :, early[1 - side]].astype(BF16)
        e[1][side].start()
    for b in range(2):
        last_far[b] = chunk_of(r_far, 3, pl.ds(b * (PW // 2), PW // 2))
    for i, here in enumerate(halves):
        for side in range(2):
            wait_far(2 * i + side)
            x_send[side, here, :] = late_rows(0, side, here).astype(BF16)
            x_two[i][side].start()

    @pl.when(far_ok)
    def _():
        for b in range(2):
            beside_copies[1 - b].wait_recv()
            send_far[3, b] = (last_far[b] + beside[b].astype(F32)).astype(BF16)

    start_far(2 * CUTS + 2)
    for side in range(2):
        send_alone(side)
    for side in range(2):
        e[0][side].wait_recv()
        e_send[4 + side] = (total[1 + side, :, early[side]] + e_recv[side].astype(F32)).astype(BF16)
        e[2][side].start()
    send_near_chunk(3)
    own_chunk(3)
    for side in range(2):
        wait_far(2 * CUTS + side)
    for i, here in enumerate(halves):
        for side in range(2):
            x_two[i][side].wait_recv()
            came = x_recv[side, here, :].astype(F32)
            x_send[4 + side, here, :] = (late_rows(1 + side, side, here) + came).astype(BF16)
            x_sum[i][side].start()
    add_near(3)
    for side in range(2):
        e[1][side].wait_recv()
        e[2][side].wait_recv()
    for side in range(2):
        out_ref[:, early[side]] = (
            total[3, :, early[side]] + e_recv[4 + side].astype(F32) + e_recv[3 - side].astype(F32)
        )
    wait_far(2 * CUTS + 2)
    for side in range(2):
        x_alone[side].wait_recv()
    for side in range(2):
        total[3, :, late[side]] = late_rows(3, side, pl.ds(0, rows)) + x_recv[3 - side].astype(F32)
    for i, here in enumerate(halves):
        for side in range(2):
            x_sum[i][side].wait_recv()
            out_ref[here, late[side]] = total[3, here, late[side]] + x_recv[4 + side, here, :].astype(F32)

    for copy in list(own_near.values()) + near_copies + e[0] + e[1] + e[2] + sum(x_two + x_sum, x_alone):
        copy.wait_send()

    @pl.when(has_r)
    def _():
        for copy in list(own_r.values()) + list(rel_r_near.values()):
            copy.wait_send()

    @pl.when(has_l)
    def _():
        for copy in list(own_l.values()) + list(rel_l_near.values()):
            copy.wait_send()

    @pl.when(far_ok)
    def _():
        for copy in list(own_far.values()) + far_copies + beside_copies:
            copy.wait_send()

        for has, relayed, turned in ((has_r, rel_r_far, turn_r), (has_l, rel_l_far, turn_l)):

            @pl.when(has)
            def _():
                for h in TURNED:
                    turned[h].wait_send()

            for h in RELAYED:
                relays = inside if h not in TO_ENDS else jnp.logical_not(ends)

                @pl.when(jnp.logical_and(has, relays))
                def _():
                    relayed[h].wait_send()

                @pl.when(jnp.logical_and(has, turned_here(h)))
                def _():
                    turned[h].wait_send()


def body(n_slab, n_cross, a_tiles, a_cols, over_tiles, over_rows, over_cols, p_tiles, p_cols):
    rows = CB * TILE // n_cross
    hbm = pl.BlockSpec(memory_space=pl.ANY)
    return pl.pallas_call(
        functools.partial(kernel, n_slab, n_cross),
        out_shape=pltpu.VMEM((rows, CW), F32),
        in_specs=[hbm] * 7,
        out_specs=pl.BlockSpec(memory_space=pltpu.VMEM),
        scratch_shapes=[
            pltpu.SMEM((NB, K), jnp.int32),
            pltpu.SMEM((OV,), jnp.int32),
            pltpu.SMEM((OV,), jnp.int32),
            pltpu.SMEM((NB, KP), jnp.int32),
            pltpu.VMEM((9, BROWS, TILE), BF16),
            pltpu.VMEM((18, TILE, WIDE), BF16),
            pltpu.VMEM((NB, K + 1, TILE, TILE), BF16),
            pltpu.VMEM((OV + 1, TILE, TILE), BF16),
            pltpu.VMEM((3, NB * TILE, WIDE), BF16),
            pltpu.VMEM((WIDE, NB * TILE), BF16),
            pltpu.VMEM((NB * TILE, PW), F32),
            pltpu.VMEM((NB * TILE, PW), BF16),
            pltpu.VMEM((n_cross, 2, rows, PW // 2), BF16),
            pltpu.VMEM((n_cross, rows, PW), BF16),
            pltpu.VMEM((n_cross, 2, rows, PW // 2), BF16),
            pltpu.VMEM((n_cross, rows, PW), BF16),
            pltpu.VMEM((2, rows, PW // 2), F32),
            pltpu.VMEM((2, rows, PW // 2), BF16),
            pltpu.VMEM((n_cross, rows, CW), F32),
            pltpu.VMEM((6, rows, EARLY // 2), BF16),
            pltpu.VMEM((6, rows, EARLY // 2), BF16),
            pltpu.VMEM((6, rows, PW // 2), BF16),
            pltpu.VMEM((6, rows, PW // 2), BF16),
            pltpu.SemaphoreType.REGULAR,
            pltpu.SemaphoreType.DMA((7,)),
            pltpu.SemaphoreType.DMA((N_SEMS,)),
            pltpu.SemaphoreType.DMA((N_SEMS,)),
        ],
        compiler_params=pltpu.CompilerParams(collective_id=0, has_side_effects=True),
    )(a_tiles, over_tiles, p_tiles.reshape(NB * KP * TILE, TILE), a_cols, over_rows, over_cols, p_cols)


def solution(mesh):
    return jax.shard_map(
        functools.partial(body, mesh.shape["slab"], mesh.shape["cross"]),
        mesh=mesh,
        in_specs=(
            P(("slab", "cross"), None, None, None),
            P(("slab", "cross"), None),
            P(("slab", "cross"), None, None),
            P(("slab", "cross")),
            P(("slab", "cross")),
            P(("slab", "cross"), None, None, None),
            P(("slab", "cross"), None),
        ),
        out_specs=P(("slab", "cross"), None),
        check_vma=False,
    )
```

```python
import functools

import jax
import jax.numpy as jnp
from jax import lax
from jax.experimental import pallas as pl
from jax.experimental.pallas import tpu as pltpu
from jax.sharding import PartitionSpec as P

CB = 2
TILE = 128
NB = 2
KP = 3
K = 7
OV = 4
WIDTH = CB * TILE
WIDE = 3 * WIDTH
PW = 5 * WIDTH
CW = 7 * WIDTH
EARLY = CW - PW
NCH = NB * KP
MARKS = 16
BROWS = MARKS + NCH * TILE
RELAYED = (0, 1, 2, 3)
TURNED = (4, 5)
TO_ENDS = (0, 1)
RUN = 16
CUTS = 2
F32 = jnp.float32
BF16 = jnp.bfloat16

OWN_R, OWN_L, OWN_NEAR, OWN_FAR, REL_L_NEAR, REL_L_FAR, REL_R_NEAR, REL_R_FAR, TURN_R, TURN_L = (
    NCH * i for i in range(10)
)
FAR0 = 10 * NCH
BESIDE = FAR0 + 2 * CUTS + 3
NEAR0 = BESIDE + 2
X0 = NEAR0 + 4
N_SEMS = X0 + 8 + 4 * CUTS


def dot(a, b):
    return lax.dot_general(a, b, (((1,), (0,)), ((), ())), preferred_element_type=F32)


def kernel(
    n_slab, n_cross,
    a_hbm, o_hbm, p_hbm, a_cols_hbm, over_rows_hbm, over_cols_hbm, p_cols_hbm,
    out_ref,
    a_cols, over_rows, over_cols, p_cols,
    halo, dense, a_in, o_in, a_dense, p_turned, acc, prod,
    send_far, send_near, recv_far, recv_near, last_far, beside, total,
    e_send, e_recv, x_send, x_recv, far_in, local_sem, send_sem, recv_sem,
):
    s = lax.axis_index("slab")
    c = lax.axis_index("cross")
    core = lax.rem(s, 2)
    near = s + 1 - 2 * core
    far = s - 1 + 2 * core
    far_ok = jnp.logical_and(far >= 0, far < n_slab)
    begins = lax.rem(s, RUN) == 0
    ends = lax.rem(s, RUN) == RUN - 1
    inside = jnp.logical_not(jnp.logical_or(begins, ends))
    far_inside = jnp.logical_and(far_ok, inside)
    far_begins = jnp.logical_and(far_ok, begins)
    far_ends = jnp.logical_and(far_ok, ends)
    right = lax.rem(c + 1, n_cross)
    left = lax.rem(c + n_cross - 1, n_cross)
    has_l = c > 0
    has_r = c < n_cross - 1
    r_near = 2 - 2 * core
    r_far = 2 * core
    rows = CB * TILE // n_cross
    part_rows = rows // CUTS

    def device(slab, cross):
        return {"slab": slab, "cross": cross}

    def remote(src, dst, i, slab, cross):
        return pltpu.make_async_remote_copy(
            src_ref=src, dst_ref=dst, send_sem=send_sem.at[i], recv_sem=recv_sem.at[i],
            device_id=device(slab, cross), device_id_type=pl.DeviceIdType.MESH,
        )

    barrier = pltpu.get_barrier_semaphore()

    def greet(slab, cross):
        pl.semaphore_signal(
            barrier, inc=1, device_id=device(slab, cross), device_id_type=pl.DeviceIdType.MESH
        )

    @pl.when(jnp.logical_and(far_ok, jnp.logical_not(ends)))
    def _():
        greet(far, c)

    greet(s, left)
    greet(s, right)
    greet(near, c)

    load_p = pltpu.make_async_copy(p_hbm, halo.at[4, pl.ds(MARKS, NCH * TILE)], local_sem.at[0])
    load_numbers = pltpu.make_async_copy(p_cols_hbm, p_cols, local_sem.at[1])
    load_a = [
        pltpu.make_async_copy(a_hbm, a_in.at[:, pl.ds(0, K)], local_sem.at[2]),
        pltpu.make_async_copy(a_cols_hbm, a_cols, local_sem.at[3]),
        pltpu.make_async_copy(o_hbm, o_in.at[pl.ds(0, OV)], local_sem.at[4]),
        pltpu.make_async_copy(over_rows_hbm, over_rows, local_sem.at[5]),
        pltpu.make_async_copy(over_cols_hbm, over_cols, local_sem.at[6]),
    ]
    for load in [load_numbers, load_p] + load_a:
        load.start()

    nothing = jnp.full((MARKS, TILE), -1.0, BF16)

    def leave_out(b):
        halo[b, pl.ds(0, MARKS), :] = nothing

    @pl.when(jnp.logical_not(has_l))
    def _():
        for r in range(3):
            leave_out(3 * r)

    @pl.when(jnp.logical_not(has_r))
    def _():
        for r in range(3):
            leave_out(3 * r + 2)

    @pl.when(jnp.logical_not(far_ok))
    def _():
        for u in range(3):
            leave_out(3 * r_far + u)
        recv_far[...] = jnp.zeros_like(recv_far)

    load_numbers.wait()
    row = lax.broadcasted_iota(jnp.int32, (MARKS, TILE), 0)
    value = jnp.full((MARKS, TILE), -1.0, F32)
    for i in range(NCH):
        value = jnp.where(row == i, p_cols[i // KP, i % KP].astype(F32), value)
    halo[4, pl.ds(0, MARKS), :] = value.astype(BF16)
    load_p.wait()
    pl.semaphore_wait(barrier, 3 + jnp.logical_and(far_ok, jnp.logical_not(begins)).astype(jnp.int32))

    @pl.when(far_ends)
    def _():
        pl.semaphore_signal(far_in, inc=1, device_id=device(far, c), device_id_type=pl.DeviceIdType.MESH)

    def halo_copies(b, to, first, slab, cross, chunks=range(NCH)):
        copies = {}
        for h in chunks:
            at = pl.ds(0, MARKS + TILE) if h == 0 else pl.ds(MARKS + h * TILE, TILE)
            copies[h] = remote(halo.at[b, at], halo.at[to, at], first + h, slab, cross)
        return copies

    own_r = halo_copies(4, 3, OWN_R, s, right)
    own_l = halo_copies(4, 5, OWN_L, s, left)
    own_near = halo_copies(4, 3 * r_far + 1, OWN_NEAR, near, c)
    own_far = halo_copies(4, 3 * r_near + 1, OWN_FAR, far, c)
    rel_l_near = halo_copies(3, 3 * r_far, REL_L_NEAR, near, c)
    rel_l_far = halo_copies(3, 3 * r_near, REL_L_FAR, far, c, RELAYED)
    rel_r_near = halo_copies(5, 3 * r_far + 2, REL_R_NEAR, near, c)
    rel_r_far = halo_copies(5, 3 * r_near + 2, REL_R_FAR, far, c, RELAYED)
    turn_r = halo_copies(3 * r_far + 1, 3 * r_far, TURN_R, s, right)
    turn_l = halo_copies(3 * r_far + 1, 3 * r_far + 2, TURN_L, s, left)

    for h in range(NCH):

        @pl.when(has_r)
        def _():
            own_r[h].start()

        @pl.when(has_l)
        def _():
            own_l[h].start()

    @pl.when(jnp.logical_and(far_ok, jnp.logical_not(begins)))
    def _():
        for h in TURNED + RELAYED:
            own_far[h].start()

    for h in range(NCH):
        own_near[h].start()

    for n in range(NB):
        a_in[n, K] = jnp.zeros((TILE, TILE), BF16)
    o_in[OV] = jnp.zeros((TILE, TILE), BF16)
    acc[...] = jnp.zeros_like(acc)
    total[...] = jnp.zeros_like(total)

    def densify(b, places=(0, 1)):
        for n in places:
            tiles, marks = [], []
            numbers = halo[b, pl.ds(0, MARKS), :].astype(F32)
            for i in range(n * KP, n * KP + KP):
                tiles.append(halo[b, pl.ds(MARKS + i * TILE, TILE), :].reshape(8, 16, TILE))
                marks.append(jnp.broadcast_to(numbers[i : i + 1], (16, TILE)).astype(BF16))
            for q in range(3 * CB):
                value = jnp.zeros((8, 16, TILE), BF16)
                for m in range(KP):
                    here = jnp.broadcast_to((marks[m] == jnp.asarray(q, BF16))[None], value.shape)
                    value = jnp.where(here, tiles[m], value)
                dense[2 * b + n, :, pl.ds(q * TILE, TILE)] = value.reshape(TILE, TILE)

    def place_a(r, places=(0, 1)):
        for n in places:
            for t in range(6 * r, 6 * r + 6):
                at = jnp.int32(K)
                for k in range(K):
                    at = jnp.where(a_cols[n, k] == t, k, at)
                value = a_in[n, at].astype(F32)
                for o in range(OV):
                    hit = jnp.logical_and(over_rows[o] == n, over_cols[o] == t)
                    value += o_in[jnp.where(hit, o, OV)].astype(F32)
                a_dense[r, pl.ds(n * TILE, TILE), pl.ds((t % 6) * TILE, TILE)] = value.astype(BF16)

    def relay(h):
        @pl.when(has_l)
        def _():
            own_r[h].wait_recv()
            if h in RELAYED:

                @pl.when(far_inside)
                def _():
                    rel_l_far[h].start()

            rel_l_near[h].start()

        @pl.when(has_r)
        def _():
            own_l[h].wait_recv()
            if h in RELAYED:

                @pl.when(far_inside)
                def _():
                    rel_r_far[h].start()

            rel_r_near[h].start()

    def turn(h):
        own_far[h].wait_recv()

        @pl.when(has_r)
        def _():
            turn_r[h].start()

        @pl.when(has_l)
        def _():
            turn_l[h].start()

    def turn_inside(h):
        @pl.when(far_inside)
        def _():
            turn(h)

    def product_of(r, u, count, j):
        right_side = dense[pl.ds(6 * r + 2 * u, 2 * count), :, pl.ds(j * WIDTH, WIDTH)]
        return dot(
            a_dense[r, :, pl.ds(u * WIDTH, count * WIDTH)], right_side.reshape(count * WIDTH, WIDTH)
        )

    def columns(r, j):
        return pl.ds(pl.multiple_of((r + j) * WIDTH, WIDTH), WIDTH)

    def add_own(r):
        densify(3 * r + 1)
        for j in range(3):
            acc[:, columns(r, j)] += product_of(r, 1, 1, j)

    def add_sides(r):
        for j in range(3):
            acc[:, columns(r, j)] += product_of(r, 0, 1, j) + product_of(r, 2, 1, j)

    near_sides = ((0, has_l, rel_l_near), (2, has_r, rel_r_near))
    far_sides = ((0, has_l, rel_l_far, turn_r), (2, has_r, rel_r_far, turn_l))
    first, rest = range(KP), range(KP, NCH)

    def near_rows(n):
        for u, has, relayed in near_sides:

            @pl.when(has)
            def _():
                for h in (first, rest)[n]:
                    relayed[h].wait_recv()

            densify(3 * r_near + u, (n,))

    def turned_here(h):
        return begins if h in TO_ENDS else jnp.logical_or(begins, ends)

    def far_rows(n):
        for u, has, relayed, turned in far_sides:

            for h in (first, rest)[n]:
                comes = jnp.logical_and(far_ok, has)
                if h in RELAYED:
                    over_slab_first = turned_here(h)

                    @pl.when(jnp.logical_and(comes, jnp.logical_not(over_slab_first)))
                    def _():
                        relayed[h].wait_recv()

                    comes = jnp.logical_and(comes, over_slab_first)

                @pl.when(comes)
                def _():
                    turned[h].wait_recv()

            densify(3 * r_far + u, (n,))

    for load in load_a:
        load.wait()
    place_a(1)
    relay(0)
    turn_inside(TURNED[0])
    add_own(1)
    relay(1)
    turn_inside(TURNED[1])
    for n in range(NB):
        for q in range(3 * CB):
            block = dense[8 + n, :, pl.ds(q * TILE, TILE)]
            p_turned[pl.ds(q * TILE, TILE), pl.ds(n * TILE, TILE)] = block.T
    place_a(0)
    relay(2)
    place_a(2)
    relay(3)
    densify(3, (0,))
    densify(5, (0,))
    for h in range(NCH):
        own_near[h].wait_recv()
    add_own(r_near)
    relay(4)
    near_rows(0)
    relay(5)

    densify(3, (1,))
    densify(5, (1,))
    add_sides(1)
    near_rows(1)
    add_sides(r_near)
    for j in range(2):
        at = pl.ds(pl.multiple_of((3 - 3 * core + j) * WIDTH, WIDTH), WIDTH)
        prod[:, at] = acc[:, at].astype(BF16)

    beyond = [h for h in range(NCH) if h not in TO_ENDS]

    @pl.when(far_begins)
    def _():
        pl.semaphore_wait(far_in, 1)
        for h in beyond:
            own_far[h].start()
        for h in TO_ENDS:
            own_far[h].start()
        for h in TO_ENDS:

            @pl.when(has_l)
            def _():
                rel_l_far[h].start()

            @pl.when(has_r)
            def _():
                rel_r_far[h].start()

        for h in TURNED + RELAYED:
            turn(h)

    @pl.when(far_ends)
    def _():
        for h in beyond:
            turn(h)
        for h in TO_ENDS:
            own_far[h].wait_recv()

    @pl.when(far_inside)
    def _():
        for h in RELAYED:
            own_far[h].wait_recv()

    add_own(r_far)
    far_rows(0)
    far_rows(1)
    for j in range(3):
        at = columns(r_far, j)
        prod[:, at] = (acc[:, at] + (product_of(r_far, 0, 1, j) + product_of(r_far, 2, 1, j))).astype(BF16)

    order = [lax.rem(c + off, n_cross) for off in (2, 1, 3, 0)]

    def chunk_of(q, k, at):
        lhs = p_turned[pl.ds(pl.multiple_of(q * WIDTH + order[k] * rows, rows), rows), :]
        return dot(lhs, prod[:, at])

    halves = [pl.ds(i * part_rows, part_rows) for i in range(CUTS)]
    pieces = [(0, b, here) for here in halves for b in range(2)]
    pieces += [(k, b, pl.ds(0, rows)) for k, b in ((1, 0), (2, 1))]
    far_copies = [
        remote(send_far.at[k, b, here], recv_far.at[k, b, here], FAR0 + i, far, c)
        for i, (k, b, here) in enumerate(pieces)
    ]
    far_copies.append(remote(send_far.at[3], recv_far.at[3], FAR0 + 2 * CUTS + 2, far, c))
    beside_copies = [
        remote(send_far.at[1 + side, 1 - side], beside.at[1 - side], BESIDE + side, s, (right, left)[side])
        for side in range(2)
    ]
    near_copies = [remote(send_near.at[k], recv_near.at[k], NEAR0 + k, near, c) for k in range(4)]

    def make_far(k, b):
        send_far[k, b] = chunk_of(r_far, k, pl.ds(b * (PW // 2), PW // 2)).astype(BF16)

    def start_far(*which):
        @pl.when(far_ok)
        def _():
            for i in which:
                far_copies[i].start()

    def send_near_chunk(k):
        for j in range(5):
            at = pl.ds(j * WIDTH, WIDTH)
            send_near[k, :, at] = chunk_of(r_near, k, at).astype(BF16)
        near_copies[k].start()

    def own_chunk(k):
        for j in range(5):
            total[k, :, pl.ds((j + 1) * WIDTH, WIDTH)] = chunk_of(1, k, pl.ds(j * WIDTH, WIDTH))

    make_far(0, 0)
    start_far(0)
    make_far(0, 1)
    start_far(*range(1, 2 * CUTS))
    for side in range(2):
        make_far(1 + side, 1 - side)

        @pl.when(far_ok)
        def _():
            beside_copies[side].start()

    send_near_chunk(0)
    for side in range(2):
        make_far(1 + side, side)
        start_far(2 * CUTS + side)
    send_near_chunk(1)
    send_near_chunk(2)
    own_chunk(0)
    own_chunk(1)
    own_chunk(2)

    near_at = pl.ds(pl.multiple_of((2 - 2 * core) * WIDTH, WIDTH), PW)
    def add_near(k):
        near_copies[k].wait_recv()
        total[k, :, near_at] += recv_near[k].astype(F32)

    def wait_far(i):
        @pl.when(far_ok)
        def _():
            far_copies[i].wait_recv()

    early_first = pl.multiple_of((5 - 5 * core) * WIDTH, WIDTH)
    late_first = pl.multiple_of(2 * core * WIDTH, WIDTH)
    early = [pl.ds(pl.multiple_of(early_first + i * (EARLY // 2), TILE), EARLY // 2) for i in range(2)]
    late = [pl.ds(pl.multiple_of(late_first + i * (PW // 2), TILE), PW // 2) for i in range(2)]

    to = [right, left]

    def early_copy(step, side):
        i = 2 * step + side
        return remote(e_send.at[i], e_recv.at[i], X0 + i, s, to[side])

    def late_copy(step, side, here, extra):
        i = 2 * step + side
        return remote(x_send.at[i, here], x_recv.at[i, here], X0 + 6 + extra + side, s, to[side])

    e = [[early_copy(step, side) for side in range(2)] for step in range(3)]
    x_two = [[late_copy(0, side, here, 2 * i) for side in range(2)] for i, here in enumerate(halves)]
    x_alone = [late_copy(1, side, pl.ds(0, rows), 2 * CUTS) for side in range(2)]
    x_sum = [[late_copy(2, side, here, 2 * CUTS + 2 + 2 * i) for side in range(2)] for i, here in enumerate(halves)]

    def late_rows(k, b, here):
        return total[k, here, late[b]] + recv_far[k, b, here, :].astype(F32)

    def send_alone(side):
        x_send[2 + side] = total[1 + side, :, late[1 - side]].astype(BF16)
        x_alone[side].start()

    add_near(0)
    for side in range(2):
        e_send[side] = total[0, :, early[side]].astype(BF16)
        e[0][side].start()
    for side in range(2):
        add_near(1 + side)
        e_send[2 + side] = total[1 + side, :, early[1 - side]].astype(BF16)
        e[1][side].start()
    for b in range(2):
        last_far[b] = chunk_of(r_far, 3, pl.ds(b * (PW // 2), PW // 2))
    for i, here in enumerate(halves):
        for side in range(2):
            wait_far(2 * i + side)
            x_send[side, here, :] = late_rows(0, side, here).astype(BF16)
            x_two[i][side].start()

    @pl.when(far_ok)
    def _():
        for b in range(2):
            beside_copies[1 - b].wait_recv()
            send_far[3, b] = (last_far[b] + beside[b].astype(F32)).astype(BF16)

    start_far(2 * CUTS + 2)
    for side in range(2):
        send_alone(side)
    for side in range(2):
        e[0][side].wait_recv()
        e_send[4 + side] = (total[1 + side, :, early[side]] + e_recv[side].astype(F32)).astype(BF16)
        e[2][side].start()
    send_near_chunk(3)
    own_chunk(3)
    for side in range(2):
        wait_far(2 * CUTS + side)
    for i, here in enumerate(halves):
        for side in range(2):
            x_two[i][side].wait_recv()
            came = x_recv[side, here, :].astype(F32)
            x_send[4 + side, here, :] = (late_rows(1 + side, side, here) + came).astype(BF16)
            x_sum[i][side].start()
    add_near(3)
    for side in range(2):
        e[1][side].wait_recv()
        e[2][side].wait_recv()
    for side in range(2):
        out_ref[:, early[side]] = (
            total[3, :, early[side]] + e_recv[4 + side].astype(F32) + e_recv[3 - side].astype(F32)
        )
    wait_far(2 * CUTS + 2)
    for side in range(2):
        x_alone[side].wait_recv()
    for side in range(2):
        total[3, :, late[side]] = late_rows(3, side, pl.ds(0, rows)) + x_recv[3 - side].astype(F32)
    for i, here in enumerate(halves):
        for side in range(2):
            x_sum[i][side].wait_recv()
            out_ref[here, late[side]] = total[3, here, late[side]] + x_recv[4 + side, here, :].astype(F32)

    for copy in list(own_near.values()) + near_copies + e[0] + e[1] + e[2] + sum(x_two + x_sum, x_alone):
        copy.wait_send()

    @pl.when(has_r)
    def _():
        for copy in list(own_r.values()) + list(rel_r_near.values()):
            copy.wait_send()

    @pl.when(has_l)
    def _():
        for copy in list(own_l.values()) + list(rel_l_near.values()):
            copy.wait_send()

    @pl.when(far_ok)
    def _():
        for copy in list(own_far.values()) + far_copies + beside_copies:
            copy.wait_send()

        for has, relayed, turned in ((has_r, rel_r_far, turn_r), (has_l, rel_l_far, turn_l)):

            @pl.when(has)
            def _():
                for h in TURNED:
                    turned[h].wait_send()

            for h in RELAYED:
                relays = inside if h not in TO_ENDS else jnp.logical_not(ends)

                @pl.when(jnp.logical_and(has, relays))
                def _():
                    relayed[h].wait_send()

                @pl.when(jnp.logical_and(has, turned_here(h)))
                def _():
                    turned[h].wait_send()


def body(n_slab, n_cross, a_tiles, a_cols, over_tiles, over_rows, over_cols, p_tiles, p_cols):
    rows = CB * TILE // n_cross
    hbm = pl.BlockSpec(memory_space=pl.ANY)
    return pl.pallas_call(
        functools.partial(kernel, n_slab, n_cross),
        out_shape=pltpu.VMEM((rows, CW), F32),
        in_specs=[hbm] * 7,
        out_specs=pl.BlockSpec(memory_space=pltpu.VMEM),
        scratch_shapes=[
            pltpu.SMEM((NB, K), jnp.int32),
            pltpu.SMEM((OV,), jnp.int32),
            pltpu.SMEM((OV,), jnp.int32),
            pltpu.SMEM((NB, KP), jnp.int32),
            pltpu.VMEM((9, BROWS, TILE), BF16),
            pltpu.VMEM((18, TILE, WIDE), BF16),
            pltpu.VMEM((NB, K + 1, TILE, TILE), BF16),
            pltpu.VMEM((OV + 1, TILE, TILE), BF16),
            pltpu.VMEM((3, NB * TILE, WIDE), BF16),
            pltpu.VMEM((WIDE, NB * TILE), BF16),
            pltpu.VMEM((NB * TILE, PW), F32),
            pltpu.VMEM((NB * TILE, PW), BF16),
            pltpu.VMEM((n_cross, 2, rows, PW // 2), BF16),
            pltpu.VMEM((n_cross, rows, PW), BF16),
            pltpu.VMEM((n_cross, 2, rows, PW // 2), BF16),
            pltpu.VMEM((n_cross, rows, PW), BF16),
            pltpu.VMEM((2, rows, PW // 2), F32),
            pltpu.VMEM((2, rows, PW // 2), BF16),
            pltpu.VMEM((n_cross, rows, CW), F32),
            pltpu.VMEM((6, rows, EARLY // 2), BF16),
            pltpu.VMEM((6, rows, EARLY // 2), BF16),
            pltpu.VMEM((6, rows, PW // 2), BF16),
            pltpu.VMEM((6, rows, PW // 2), BF16),
            pltpu.SemaphoreType.REGULAR,
            pltpu.SemaphoreType.DMA((7,)),
            pltpu.SemaphoreType.DMA((N_SEMS,)),
            pltpu.SemaphoreType.DMA((N_SEMS,)),
        ],
        compiler_params=pltpu.CompilerParams(collective_id=0, has_side_effects=True),
    )(a_tiles, over_tiles, p_tiles.reshape(NB * KP * TILE, TILE), a_cols, over_rows, over_cols, p_cols)


def solution(mesh):
    return jax.shard_map(
        functools.partial(body, mesh.shape["slab"], mesh.shape["cross"]),
        mesh=mesh,
        in_specs=(
            P(("slab", "cross"), None, None, None),
            P(("slab", "cross"), None),
            P(("slab", "cross"), None, None),
            P(("slab", "cross")),
            P(("slab", "cross")),
            P(("slab", "cross"), None, None, None),
            P(("slab", "cross"), None),
        ),
        out_specs=P(("slab", "cross"), None),
        check_vma=False,
    )
```

```python
import functools

import jax
import jax.numpy as jnp
from jax import lax
from jax.experimental import pallas as pl
from jax.experimental.pallas import tpu as pltpu
from jax.sharding import PartitionSpec as P

CB = 2
TILE = 128
NB = 2
KP = 3
K = 7
OV = 4
WIDTH = CB * TILE
WIDE = 3 * WIDTH
PW = 5 * WIDTH
CW = 7 * WIDTH
EARLY = CW - PW
NCH = NB * KP
MARKS = 16
BROWS = MARKS + NCH * TILE
RELAYED = (0, 1, 2, 3)
TURNED = (4, 5)
TO_ENDS = (0, 1)
RUN = 16
CUTS = 2
F32 = jnp.float32
BF16 = jnp.bfloat16

OWN_R, OWN_L, OWN_NEAR, OWN_FAR, REL_L_NEAR, REL_L_FAR, REL_R_NEAR, REL_R_FAR, TURN_R, TURN_L = (
    NCH * i for i in range(10)
)
FAR0 = 10 * NCH
BESIDE = FAR0 + 2 * CUTS + 3
NEAR0 = BESIDE + 2
X0 = NEAR0 + 4
N_SEMS = X0 + 8 + 4 * CUTS


def dot(a, b):
    return lax.dot_general(a, b, (((1,), (0,)), ((), ())), preferred_element_type=F32)


def kernel(
    n_slab, n_cross,
    a_hbm, o_hbm, p_hbm, a_cols_hbm, over_rows_hbm, over_cols_hbm, p_cols_hbm,
    out_ref,
    a_cols, over_rows, over_cols, p_cols,
    halo, dense, a_in, o_in, a_dense, p_turned, acc, prod,
    send_far, send_near, recv_far, recv_near, last_far, beside, total,
    e_send, e_recv, x_send, x_recv, far_in, local_sem, send_sem, recv_sem,
):
    s = lax.axis_index("slab")
    c = lax.axis_index("cross")
    core = lax.rem(s, 2)
    near = s + 1 - 2 * core
    far = s - 1 + 2 * core
    far_ok = jnp.logical_and(far >= 0, far < n_slab)
    begins = lax.rem(s, RUN) == 0
    ends = lax.rem(s, RUN) == RUN - 1
    inside = jnp.logical_not(jnp.logical_or(begins, ends))
    far_inside = jnp.logical_and(far_ok, inside)
    far_begins = jnp.logical_and(far_ok, begins)
    far_ends = jnp.logical_and(far_ok, ends)
    right = lax.rem(c + 1, n_cross)
    left = lax.rem(c + n_cross - 1, n_cross)
    has_l = c > 0
    has_r = c < n_cross - 1
    r_near = 2 - 2 * core
    r_far = 2 * core
    rows = CB * TILE // n_cross
    part_rows = rows // CUTS

    def device(slab, cross):
        return {"slab": slab, "cross": cross}

    def remote(src, dst, i, slab, cross):
        return pltpu.make_async_remote_copy(
            src_ref=src, dst_ref=dst, send_sem=send_sem.at[i], recv_sem=recv_sem.at[i],
            device_id=device(slab, cross), device_id_type=pl.DeviceIdType.MESH,
        )

    barrier = pltpu.get_barrier_semaphore()

    def greet(slab, cross):
        pl.semaphore_signal(
            barrier, inc=1, device_id=device(slab, cross), device_id_type=pl.DeviceIdType.MESH
        )

    @pl.when(jnp.logical_and(far_ok, jnp.logical_not(ends)))
    def _():
        greet(far, c)

    greet(s, left)
    greet(s, right)
    greet(near, c)

    load_p = pltpu.make_async_copy(p_hbm, halo.at[4, pl.ds(MARKS, NCH * TILE)], local_sem.at[0])
    load_numbers = pltpu.make_async_copy(p_cols_hbm, p_cols, local_sem.at[1])
    load_a = [
        pltpu.make_async_copy(a_hbm, a_in.at[:, pl.ds(0, K)], local_sem.at[2]),
        pltpu.make_async_copy(a_cols_hbm, a_cols, local_sem.at[3]),
        pltpu.make_async_copy(o_hbm, o_in.at[pl.ds(0, OV)], local_sem.at[4]),
        pltpu.make_async_copy(over_rows_hbm, over_rows, local_sem.at[5]),
        pltpu.make_async_copy(over_cols_hbm, over_cols, local_sem.at[6]),
    ]
    for load in [load_numbers, load_p] + load_a:
        load.start()

    nothing = jnp.full((MARKS, TILE), -1.0, BF16)

    def leave_out(b):
        halo[b, pl.ds(0, MARKS), :] = nothing

    @pl.when(jnp.logical_not(has_l))
    def _():
        for r in range(3):
            leave_out(3 * r)

    @pl.when(jnp.logical_not(has_r))
    def _():
        for r in range(3):
            leave_out(3 * r + 2)

    @pl.when(jnp.logical_not(far_ok))
    def _():
        for u in range(3):
            leave_out(3 * r_far + u)
        recv_far[...] = jnp.zeros_like(recv_far)

    load_numbers.wait()
    row = lax.broadcasted_iota(jnp.int32, (MARKS, TILE), 0)
    value = jnp.full((MARKS, TILE), -1.0, F32)
    for i in range(NCH):
        value = jnp.where(row == i, p_cols[i // KP, i % KP].astype(F32), value)
    halo[4, pl.ds(0, MARKS), :] = value.astype(BF16)
    load_p.wait()
    pl.semaphore_wait(barrier, 3 + jnp.logical_and(far_ok, jnp.logical_not(begins)).astype(jnp.int32))

    @pl.when(far_ends)
    def _():
        pl.semaphore_signal(far_in, inc=1, device_id=device(far, c), device_id_type=pl.DeviceIdType.MESH)

    def halo_copies(b, to, first, slab, cross, chunks=range(NCH)):
        copies = {}
        for h in chunks:
            at = pl.ds(0, MARKS + TILE) if h == 0 else pl.ds(MARKS + h * TILE, TILE)
            copies[h] = remote(halo.at[b, at], halo.at[to, at], first + h, slab, cross)
        return copies

    own_r = halo_copies(4, 3, OWN_R, s, right)
    own_l = halo_copies(4, 5, OWN_L, s, left)
    own_near = halo_copies(4, 3 * r_far + 1, OWN_NEAR, near, c)
    own_far = halo_copies(4, 3 * r_near + 1, OWN_FAR, far, c)
    rel_l_near = halo_copies(3, 3 * r_far, REL_L_NEAR, near, c)
    rel_l_far = halo_copies(3, 3 * r_near, REL_L_FAR, far, c, RELAYED)
    rel_r_near = halo_copies(5, 3 * r_far + 2, REL_R_NEAR, near, c)
    rel_r_far = halo_copies(5, 3 * r_near + 2, REL_R_FAR, far, c, RELAYED)
    turn_r = halo_copies(3 * r_far + 1, 3 * r_far, TURN_R, s, right)
    turn_l = halo_copies(3 * r_far + 1, 3 * r_far + 2, TURN_L, s, left)

    for h in range(NCH):

        @pl.when(has_r)
        def _():
            own_r[h].start()

        @pl.when(has_l)
        def _():
            own_l[h].start()

    @pl.when(jnp.logical_and(far_ok, jnp.logical_not(begins)))
    def _():
        for h in TURNED + RELAYED:
            own_far[h].start()

    for h in range(NCH):
        own_near[h].start()

    for n in range(NB):
        a_in[n, K] = jnp.zeros((TILE, TILE), BF16)
    o_in[OV] = jnp.zeros((TILE, TILE), BF16)
    acc[...] = jnp.zeros_like(acc)
    total[...] = jnp.zeros_like(total)

    def densify(b, places=(0, 1)):
        for n in places:
            tiles, marks = [], []
            numbers = halo[b, pl.ds(0, MARKS), :].astype(F32)
            for i in range(n * KP, n * KP + KP):
                tiles.append(halo[b, pl.ds(MARKS + i * TILE, TILE), :].reshape(8, 16, TILE))
                marks.append(jnp.broadcast_to(numbers[i : i + 1], (16, TILE)).astype(BF16))
            for q in range(3 * CB):
                value = jnp.zeros((8, 16, TILE), BF16)
                for m in range(KP):
                    here = jnp.broadcast_to((marks[m] == jnp.asarray(q, BF16))[None], value.shape)
                    value = jnp.where(here, tiles[m], value)
                dense[2 * b + n, :, pl.ds(q * TILE, TILE)] = value.reshape(TILE, TILE)

    def place_a(r, places=(0, 1)):
        for n in places:
            for t in range(6 * r, 6 * r + 6):
                at = jnp.int32(K)
                for k in range(K):
                    at = jnp.where(a_cols[n, k] == t, k, at)
                value = a_in[n, at].astype(F32)
                for o in range(OV):
                    hit = jnp.logical_and(over_rows[o] == n, over_cols[o] == t)
                    value += o_in[jnp.where(hit, o, OV)].astype(F32)
                a_dense[r, pl.ds(n * TILE, TILE), pl.ds((t % 6) * TILE, TILE)] = value.astype(BF16)

    def relay(h):
        @pl.when(has_l)
        def _():
            own_r[h].wait_recv()
            if h in RELAYED:

                @pl.when(far_inside)
                def _():
                    rel_l_far[h].start()

            rel_l_near[h].start()

        @pl.when(has_r)
        def _():
            own_l[h].wait_recv()
            if h in RELAYED:

                @pl.when(far_inside)
                def _():
                    rel_r_far[h].start()

            rel_r_near[h].start()

    def turn(h):
        own_far[h].wait_recv()

        @pl.when(has_r)
        def _():
            turn_r[h].start()

        @pl.when(has_l)
        def _():
            turn_l[h].start()

    def turn_inside(h):
        @pl.when(far_inside)
        def _():
            turn(h)

    def product_of(r, u, count, j):
        right_side = dense[pl.ds(6 * r + 2 * u, 2 * count), :, pl.ds(j * WIDTH, WIDTH)]
        return dot(
            a_dense[r, :, pl.ds(u * WIDTH, count * WIDTH)], right_side.reshape(count * WIDTH, WIDTH)
        )

    def columns(r, j):
        return pl.ds(pl.multiple_of((r + j) * WIDTH, WIDTH), WIDTH)

    def add_own(r):
        densify(3 * r + 1)
        for j in range(3):
            acc[:, columns(r, j)] += product_of(r, 1, 1, j)

    def add_sides(r):
        for j in range(3):
            acc[:, columns(r, j)] += product_of(r, 0, 1, j) + product_of(r, 2, 1, j)

    near_sides = ((0, has_l, rel_l_near), (2, has_r, rel_r_near))
    far_sides = ((0, has_l, rel_l_far, turn_r), (2, has_r, rel_r_far, turn_l))
    first, rest = range(KP), range(KP, NCH)

    def near_rows(n):
        for u, has, relayed in near_sides:

            @pl.when(has)
            def _():
                for h in (first, rest)[n]:
                    relayed[h].wait_recv()

            densify(3 * r_near + u, (n,))

    def turned_here(h):
        return begins if h in TO_ENDS else jnp.logical_or(begins, ends)

    def far_rows(n):
        for u, has, relayed, turned in far_sides:

            for h in (first, rest)[n]:
                comes = jnp.logical_and(far_ok, has)
                if h in RELAYED:
                    over_slab_first = turned_here(h)

                    @pl.when(jnp.logical_and(comes, jnp.logical_not(over_slab_first)))
                    def _():
                        relayed[h].wait_recv()

                    comes = jnp.logical_and(comes, over_slab_first)

                @pl.when(comes)
                def _():
                    turned[h].wait_recv()

            densify(3 * r_far + u, (n,))

    for load in load_a:
        load.wait()
    place_a(1)
    relay(0)
    turn_inside(TURNED[0])
    add_own(1)
    relay(1)
    turn_inside(TURNED[1])
    for n in range(NB):
        for q in range(3 * CB):
            block = dense[8 + n, :, pl.ds(q * TILE, TILE)]
            p_turned[pl.ds(q * TILE, TILE), pl.ds(n * TILE, TILE)] = block.T
    place_a(0)
    relay(2)
    place_a(2)
    relay(3)
    densify(3, (0,))
    densify(5, (0,))
    for h in range(NCH):
        own_near[h].wait_recv()
    add_own(r_near)
    relay(4)
    near_rows(0)
    relay(5)

    densify(3, (1,))
    densify(5, (1,))
    add_sides(1)
    beyond = [h for h in range(NCH) if h not in TO_ENDS]

    @pl.when(far_begins)
    def _():
        pl.semaphore_wait(far_in, 1)
        for h in beyond:
            own_far[h].start()
        for h in TO_ENDS:
            own_far[h].start()
        for h in TO_ENDS:

            @pl.when(has_l)
            def _():
                rel_l_far[h].start()

            @pl.when(has_r)
            def _():
                rel_r_far[h].start()

        for h in TURNED + RELAYED:
            turn(h)

    @pl.when(far_ends)
    def _():
        for h in beyond:
            turn(h)
        for h in TO_ENDS:
            own_far[h].wait_recv()

    @pl.when(far_inside)
    def _():
        for h in RELAYED:
            own_far[h].wait_recv()

    add_own(r_far)
    near_rows(1)
    add_sides(r_near)
    for j in range(2):
        at = pl.ds(pl.multiple_of((3 - 3 * core + j) * WIDTH, WIDTH), WIDTH)
        prod[:, at] = acc[:, at].astype(BF16)

    far_rows(0)
    far_rows(1)
    for j in range(3):
        at = columns(r_far, j)
        prod[:, at] = (acc[:, at] + (product_of(r_far, 0, 1, j) + product_of(r_far, 2, 1, j))).astype(BF16)

    order = [lax.rem(c + off, n_cross) for off in (2, 1, 3, 0)]

    def chunk_of(q, k, at):
        lhs = p_turned[pl.ds(pl.multiple_of(q * WIDTH + order[k] * rows, rows), rows), :]
        return dot(lhs, prod[:, at])

    halves = [pl.ds(i * part_rows, part_rows) for i in range(CUTS)]
    pieces = [(0, b, here) for here in halves for b in range(2)]
    pieces += [(k, b, pl.ds(0, rows)) for k, b in ((1, 0), (2, 1))]
    far_copies = [
        remote(send_far.at[k, b, here], recv_far.at[k, b, here], FAR0 + i, far, c)
        for i, (k, b, here) in enumerate(pieces)
    ]
    far_copies.append(remote(send_far.at[3], recv_far.at[3], FAR0 + 2 * CUTS + 2, far, c))
    beside_copies = [
        remote(send_far.at[1 + side, 1 - side], beside.at[1 - side], BESIDE + side, s, (right, left)[side])
        for side in range(2)
    ]
    near_copies = [remote(send_near.at[k], recv_near.at[k], NEAR0 + k, near, c) for k in range(4)]

    def make_far(k, b):
        send_far[k, b] = chunk_of(r_far, k, pl.ds(b * (PW // 2), PW // 2)).astype(BF16)

    def start_far(*which):
        @pl.when(far_ok)
        def _():
            for i in which:
                far_copies[i].start()

    def send_near_chunk(k):
        for j in range(5):
            at = pl.ds(j * WIDTH, WIDTH)
            send_near[k, :, at] = chunk_of(r_near, k, at).astype(BF16)
        near_copies[k].start()

    def own_chunk(k):
        for j in range(5):
            total[k, :, pl.ds((j + 1) * WIDTH, WIDTH)] = chunk_of(1, k, pl.ds(j * WIDTH, WIDTH))

    make_far(0, 0)
    make_far(0, 1)
    start_far(*range(2 * CUTS))
    for side in range(2):
        make_far(1 + side, 1 - side)

        @pl.when(far_ok)
        def _():
            beside_copies[side].start()

    send_near_chunk(0)
    for side in range(2):
        make_far(1 + side, side)
        start_far(2 * CUTS + side)
    send_near_chunk(1)
    send_near_chunk(2)
    own_chunk(0)
    own_chunk(1)
    own_chunk(2)

    near_at = pl.ds(pl.multiple_of((2 - 2 * core) * WIDTH, WIDTH), PW)
    def add_near(k):
        near_copies[k].wait_recv()
        total[k, :, near_at] += recv_near[k].astype(F32)

    def wait_far(i):
        @pl.when(far_ok)
        def _():
            far_copies[i].wait_recv()

    early_first = pl.multiple_of((5 - 5 * core) * WIDTH, WIDTH)
    late_first = pl.multiple_of(2 * core * WIDTH, WIDTH)
    early = [pl.ds(pl.multiple_of(early_first + i * (EARLY // 2), TILE), EARLY // 2) for i in range(2)]
    late = [pl.ds(pl.multiple_of(late_first + i * (PW // 2), TILE), PW // 2) for i in range(2)]

    to = [right, left]

    def early_copy(step, side):
        i = 2 * step + side
        return remote(e_send.at[i], e_recv.at[i], X0 + i, s, to[side])

    def late_copy(step, side, here, extra):
        i = 2 * step + side
        return remote(x_send.at[i, here], x_recv.at[i, here], X0 + 6 + extra + side, s, to[side])

    e = [[early_copy(step, side) for side in range(2)] for step in range(3)]
    x_two = [[late_copy(0, side, here, 2 * i) for side in range(2)] for i, here in enumerate(halves)]
    x_alone = [late_copy(1, side, pl.ds(0, rows), 2 * CUTS) for side in range(2)]
    x_sum = [[late_copy(2, side, here, 2 * CUTS + 2 + 2 * i) for side in range(2)] for i, here in enumerate(halves)]

    def late_rows(k, b, here):
        return total[k, here, late[b]] + recv_far[k, b, here, :].astype(F32)

    def send_alone(side):
        x_send[2 + side] = total[1 + side, :, late[1 - side]].astype(BF16)
        x_alone[side].start()

    add_near(0)
    for side in range(2):
        e_send[side] = total[0, :, early[side]].astype(BF16)
        e[0][side].start()
    for side in range(2):
        add_near(1 + side)
        e_send[2 + side] = total[1 + side, :, early[1 - side]].astype(BF16)
        e[1][side].start()
    for b in range(2):
        last_far[b] = chunk_of(r_far, 3, pl.ds(b * (PW // 2), PW // 2))
    for i, here in enumerate(halves):
        for side in range(2):
            wait_far(2 * i + side)
            x_send[side, here, :] = late_rows(0, side, here).astype(BF16)
            x_two[i][side].start()

    @pl.when(far_ok)
    def _():
        for b in range(2):
            beside_copies[1 - b].wait_recv()
            send_far[3, b] = (last_far[b] + beside[b].astype(F32)).astype(BF16)

    start_far(2 * CUTS + 2)
    for side in range(2):
        send_alone(side)
    for side in range(2):
        e[0][side].wait_recv()
        e_send[4 + side] = (total[1 + side, :, early[side]] + e_recv[side].astype(F32)).astype(BF16)
        e[2][side].start()
    send_near_chunk(3)
    own_chunk(3)
    for side in range(2):
        wait_far(2 * CUTS + side)
    for i, here in enumerate(halves):
        for side in range(2):
            x_two[i][side].wait_recv()
            came = x_recv[side, here, :].astype(F32)
            x_send[4 + side, here, :] = (late_rows(1 + side, side, here) + came).astype(BF16)
            x_sum[i][side].start()
    add_near(3)
    for side in range(2):
        e[1][side].wait_recv()
        e[2][side].wait_recv()
    for side in range(2):
        out_ref[:, early[side]] = (
            total[3, :, early[side]] + e_recv[4 + side].astype(F32) + e_recv[3 - side].astype(F32)
        )
    wait_far(2 * CUTS + 2)
    for side in range(2):
        x_alone[side].wait_recv()
    for side in range(2):
        total[3, :, late[side]] = late_rows(3, side, pl.ds(0, rows)) + x_recv[3 - side].astype(F32)
    for i, here in enumerate(halves):
        for side in range(2):
            x_sum[i][side].wait_recv()
            out_ref[here, late[side]] = total[3, here, late[side]] + x_recv[4 + side, here, :].astype(F32)

    for copy in list(own_near.values()) + near_copies + e[0] + e[1] + e[2] + sum(x_two + x_sum, x_alone):
        copy.wait_send()

    @pl.when(has_r)
    def _():
        for copy in list(own_r.values()) + list(rel_r_near.values()):
            copy.wait_send()

    @pl.when(has_l)
    def _():
        for copy in list(own_l.values()) + list(rel_l_near.values()):
            copy.wait_send()

    @pl.when(far_ok)
    def _():
        for copy in list(own_far.values()) + far_copies + beside_copies:
            copy.wait_send()

        for has, relayed, turned in ((has_r, rel_r_far, turn_r), (has_l, rel_l_far, turn_l)):

            @pl.when(has)
            def _():
                for h in TURNED:
                    turned[h].wait_send()

            for h in RELAYED:
                relays = inside if h not in TO_ENDS else jnp.logical_not(ends)

                @pl.when(jnp.logical_and(has, relays))
                def _():
                    relayed[h].wait_send()

                @pl.when(jnp.logical_and(has, turned_here(h)))
                def _():
                    turned[h].wait_send()


def body(n_slab, n_cross, a_tiles, a_cols, over_tiles, over_rows, over_cols, p_tiles, p_cols):
    rows = CB * TILE // n_cross
    hbm = pl.BlockSpec(memory_space=pl.ANY)
    return pl.pallas_call(
        functools.partial(kernel, n_slab, n_cross),
        out_shape=pltpu.VMEM((rows, CW), F32),
        in_specs=[hbm] * 7,
        out_specs=pl.BlockSpec(memory_space=pltpu.VMEM),
        scratch_shapes=[
            pltpu.SMEM((NB, K), jnp.int32),
            pltpu.SMEM((OV,), jnp.int32),
            pltpu.SMEM((OV,), jnp.int32),
            pltpu.SMEM((NB, KP), jnp.int32),
            pltpu.VMEM((9, BROWS, TILE), BF16),
            pltpu.VMEM((18, TILE, WIDE), BF16),
            pltpu.VMEM((NB, K + 1, TILE, TILE), BF16),
            pltpu.VMEM((OV + 1, TILE, TILE), BF16),
            pltpu.VMEM((3, NB * TILE, WIDE), BF16),
            pltpu.VMEM((WIDE, NB * TILE), BF16),
            pltpu.VMEM((NB * TILE, PW), F32),
            pltpu.VMEM((NB * TILE, PW), BF16),
            pltpu.VMEM((n_cross, 2, rows, PW // 2), BF16),
            pltpu.VMEM((n_cross, rows, PW), BF16),
            pltpu.VMEM((n_cross, 2, rows, PW // 2), BF16),
            pltpu.VMEM((n_cross, rows, PW), BF16),
            pltpu.VMEM((2, rows, PW // 2), F32),
            pltpu.VMEM((2, rows, PW // 2), BF16),
            pltpu.VMEM((n_cross, rows, CW), F32),
            pltpu.VMEM((6, rows, EARLY // 2), BF16),
            pltpu.VMEM((6, rows, EARLY // 2), BF16),
            pltpu.VMEM((6, rows, PW // 2), BF16),
            pltpu.VMEM((6, rows, PW // 2), BF16),
            pltpu.SemaphoreType.REGULAR,
            pltpu.SemaphoreType.DMA((7,)),
            pltpu.SemaphoreType.DMA((N_SEMS,)),
            pltpu.SemaphoreType.DMA((N_SEMS,)),
        ],
        compiler_params=pltpu.CompilerParams(collective_id=0, has_side_effects=True),
    )(a_tiles, over_tiles, p_tiles.reshape(NB * KP * TILE, TILE), a_cols, over_rows, over_cols, p_cols)


def solution(mesh):
    return jax.shard_map(
        functools.partial(body, mesh.shape["slab"], mesh.shape["cross"]),
        mesh=mesh,
        in_specs=(
            P(("slab", "cross"), None, None, None),
            P(("slab", "cross"), None),
            P(("slab", "cross"), None, None),
            P(("slab", "cross")),
            P(("slab", "cross")),
            P(("slab", "cross"), None, None, None),
            P(("slab", "cross"), None),
        ),
        out_specs=P(("slab", "cross"), None),
        check_vma=False,
    )
```
